128 devices in a mesh: gx: 8 (over z, core), gy: 16 (over x, y).
Axes of the slice: x: 4, y: 4, z: 4, core: 2. Of those that a mesh axis runs over, the one named last changes fastest.
Arguments:
- density: float32 [8, 1024, 4096], P(None, 'gy', 'gx'), may hold values from -6 to 6
- tracer: float32 [8, 1024, 4096], P(None, 'gy', 'gx'), may hold values from -6 to 6
- sea_mask: int32 [1024, 4096], P('gy', 'gx'), may hold values 0 or 1
- mixed_level: int32 [1024, 4096], P('gy', 'gx'), may hold values from 0 to 4
- tile_blocks: int32 [128], replicated, may hold values from 0 to 127, each once
- block_owner: int32 [128], replicated, may hold values from 0 to 127, as said below
Outputs:
- tracer_out: float32 [8, 1024, 4096], P(None, 'gy', 'gx')
The draws below stay inside these ranges and needn't reach their ends.
Inputs may be any that keep to these rules, and one draw needn't show every extreme that they name: `sea_mask`: 1 marks sea, 0 land. `tile_blocks`: each of the 128 blocks once. `block_owner`: each of the 128 dynamics slots once; slot t belongs to gy index t // 8; of the 8 physics slots of one gy index, at most 2 go to any one gy index, and exactly 2 to every gy index that they reach.
All inputs are finite; a program needn't handle non-finite values. No bound on the sum of `sea_mask` on one device may be relied on, other than what follows from the above.
Results may differ from the reference program's by a relative error of at most 0.0003.
Values sent between devices are 32-bit elements; how exact they have to be, the bound alone decides.
No kernel may reach another device: no remote copies, remote signals or barrier semaphores. Data moves between devices by JAX's collectives and lax.ppermute only.
A program may use at most 128 MiB of HBM per device.

```python
import jax
import jax.numpy as jnp
from jax import lax

K = 8
BR = 8
BPD = 8
CAP = 2
ITERS = 4
NBLK = 128
NY = 1024
NX = 4096


def draw_block_owner(key, part):
    devices = NBLK // BPD
    key_offsets, key_order, key_shuffle, key_places = jax.random.split(key, 4)
    distinct = jax.random.permutation(key_offsets, devices)[:BPD // CAP]
    offsets = jax.random.permutation(key_order, jnp.repeat(distinct, CAP))
    shuffle = jax.random.permutation(key_shuffle, devices)
    places = jax.random.permutation(key_places, BPD)
    sources = jnp.arange(devices, dtype=jnp.int32)[:, None]
    targets = jnp.take(shuffle, (sources + offsets[None, :]) % devices)
    return (targets * BPD + places[None, :]).reshape(-1).astype(jnp.int32)


def set_ends(entries, own_key, low, high):
    longest = entries.shape.index(max(entries.shape))
    spots = []
    for shift in (0, 1):
        where = [jax.random.randint(jax.random.fold_in(own_key, axis), (), 0, length) for axis, length in enumerate(entries.shape)]
        where[longest] = (where[longest] + shift) % entries.shape[longest]
        spots.append(tuple(where))
    return entries.at[spots[0]].set(low).at[spots[1]].set(high)


def block_levels(stream_key, shape, pieces, smallest, high):
    level, own = 1.0, jax.random.fold_in(stream_key, 6)
    for axis_at, blocks in pieces:
        steps = jnp.exp(jax.random.uniform(jax.random.fold_in(own, axis_at), (blocks,), jnp.float32, smallest / len(pieces), high / len(pieces)))
        level = level * jnp.repeat(steps, shape[axis_at] // blocks).reshape([-1 if axis == axis_at else 1 for axis in range(len(shape))])
    return level


def noise(rng, shape, spread, most, shards=(), kind=jnp.bfloat16):
    values = jax.random.normal(rng, shape, jnp.float32) * spread
    if len(shards) > 0:
        values = block_levels(rng, shape, shards, -0.22, 0.18) * values
    return jnp.clip(values, min=-most, max=most).astype(kind)


def setup_inputs(seed: int = 0) -> dict:
    key_of = jax.random.split(jax.random.key(seed), 7)
    density = noise(key_of[0], (K, NY, NX), 1.0, 6.0, ((1, 16), (2, 8)), jnp.float32)
    tracer = noise(key_of[1], (K, NY, NX), 1.0, 6.0, ((1, 16), (2, 8)), jnp.float32)
    sea_mask = set_ends((jax.random.randint(key_of[2], (NY, NX), 0, 4) < 3).astype(jnp.int32), jax.random.fold_in(key_of[2], 1), 0, 1)
    mixed_level = set_ends(jax.random.randint(key_of[3], (NY, NX), 0, K // 2 + 1), jax.random.fold_in(key_of[3], 1), 0, (K // 2 + 1) - 1).astype(jnp.int32)
    tile_blocks = jax.random.permutation(key_of[4], NBLK).astype(jnp.int32)
    block_owner = draw_block_owner(jax.random.fold_in(key_of[6], 71), 0)
    return {"density": density, "tracer": tracer, "sea_mask": sea_mask, "mixed_level": mixed_level, "tile_blocks": tile_blocks, "block_owner": block_owner}


TIME_STEP = 0.2
STRATIFICATION = 1.0
DENSITY_FLOOR = 0.25
SLOPE_LIMIT = 1.0
TAPER_WIDTH = 0.5
KERNEL_OFFSET = 0.05
BASE_DIFFUSIVITY = 0.2
VISBECK_ALPHA = 0.5

def interior(quantity):
    return quantity[..., 1:-1, 1:-1]

def masked_steps(quantity, seawater):
    across_east = seawater[..., :, 1:] * seawater[..., :, :-1]
    across_north = seawater[..., 1:, :] * seawater[..., :-1, :]
    step_east = (quantity[..., :, 1:] - quantity[..., :, :-1]) * across_east
    step_north = (quantity[..., 1:, :] - quantity[..., :-1, :]) * across_north
    return (step_east, step_north)

def centered_east(step_east):
    return 0.5 * (step_east[..., 1:-1, 1:] + step_east[..., 1:-1, :-1])

def centered_north(step_north):
    return 0.5 * (step_north[..., 1:, 1:-1] + step_north[..., :-1, 1:-1])

def vertical_center(quantity):
    shallower = jnp.concatenate([quantity[:1], quantity[:-1]], axis=0)
    deeper = jnp.concatenate([quantity[1:], quantity[-1:]], axis=0)
    return 0.5 * (deeper - shallower)

def vertical_divergence(column_flux):
    zero_layer = jnp.zeros_like(column_flux[:1])
    shallower = jnp.concatenate([zero_layer, column_flux[:-1]], axis=0)
    deeper = jnp.concatenate([column_flux[1:], zero_layer], axis=0)
    return 0.5 * (deeper - shallower)

def physics(density_rim, seawater_rim, mixed_depth):
    level_count = density_rim.shape[0]
    levels = jnp.arange(level_count, dtype=jnp.float32).reshape(-1, 1, 1, 1)
    step_east, step_north = masked_steps(density_rim, seawater_rim)
    grad_east = centered_east(step_east)
    grad_north = centered_north(step_north)
    stratified = vertical_center(interior(density_rim) + STRATIFICATION * levels)
    denominator = jnp.maximum(stratified, DENSITY_FLOOR)
    slope_east = -grad_east / denominator
    slope_north = -grad_north / denominator
    squared = slope_east * slope_east + slope_north * slope_north
    taper_factor = 0.5 * (1.0 + jnp.tanh((SLOPE_LIMIT - squared) / TAPER_WIDTH))
    surface = jnp.minimum(1.0, (levels + 1.0) / (mixed_depth + 1.0))
    seawater = interior(seawater_rim)
    factor = taper_factor * surface * seawater
    slope_east = slope_east * factor
    slope_north = slope_north * factor
    tapered_sq = slope_east * slope_east + slope_north * slope_north
    below_layer = (levels >= mixed_depth).astype(jnp.float32)
    kernel = jnp.sqrt(denominator * (tapered_sq + KERNEL_OFFSET)) * below_layer
    depth_count = level_count - mixed_depth
    diffusivity = seawater * (BASE_DIFFUSIVITY + VISBECK_ALPHA * lax.optimization_barrier(jnp.sum(kernel, axis=0)) / depth_count)
    return (slope_east, slope_north, diffusivity)

def advance(tracer_rim, east_rim, north_rim, diffusivity_rim, seawater_rim):
    step_east, step_north = masked_steps(tracer_rim, seawater_rim)
    face_east = 0.5 * (diffusivity_rim[..., :, 1:] + diffusivity_rim[..., :, :-1]) * step_east
    face_north = 0.5 * (diffusivity_rim[..., 1:, :] + diffusivity_rim[..., :-1, :]) * step_north
    lateral = face_east[..., 1:-1, 1:] - face_east[..., 1:-1, :-1] + (face_north[..., 1:, 1:-1] - face_north[..., :-1, 1:-1])
    grad_east = centered_east(step_east)
    grad_north = centered_north(step_north)
    center_tracer = interior(tracer_rim)
    grad_down = vertical_center(center_tracer)
    slope_east = interior(east_rim)
    slope_north = interior(north_rim)
    column_flux = interior(diffusivity_rim) * (2.0 * slope_east * grad_east + 2.0 * slope_north * grad_north + (slope_east * slope_east + slope_north * slope_north) * grad_down)
    tendency = (lateral + vertical_divergence(column_flux)) * interior(seawater_rim)
    return center_tracer + TIME_STEP * tendency

def with_rim(quantity):
    leading = quantity.ndim - 2
    padded = jnp.pad(quantity, [(0, 0)] * leading + [(1, 1), (0, 0)])
    return jnp.pad(padded, [(0, 0)] * (leading + 1) + [(1, 1)], mode='wrap')

def reorder(quantity, ordering):
    leading = quantity.shape[:-2]
    blocks = quantity.reshape(leading + (ordering.shape[0], BR, quantity.shape[-1]))
    picked = jnp.take(blocks, ordering, axis=len(leading))
    return picked.reshape(quantity.shape)

def reference(density, tracer, sea_mask, mixed_level, tile_blocks, block_owner):
    physics_slot = jnp.argsort(tile_blocks).astype(jnp.int32)
    dynamics_blocks = jnp.take(tile_blocks, jnp.argsort(block_owner).astype(jnp.int32)).astype(jnp.int32)
    dynamics_slot = jnp.argsort(dynamics_blocks).astype(jnp.int32)
    density_grid = reorder(density, physics_slot)
    seawater = reorder(sea_mask, physics_slot).astype(jnp.float32)
    mixed_depth = reorder(mixed_level, physics_slot).astype(jnp.float32)
    seawater_rim = with_rim(seawater[None])
    slope_east, slope_north, diffusivity = physics(with_rim(density_grid[:, None]), seawater_rim, mixed_depth[None])
    diffusivity_rim = with_rim(diffusivity)
    east_rim = with_rim(slope_east)
    north_rim = with_rim(slope_north)
    current = reorder(tracer, dynamics_slot)[:, None]
    for sweep_index in range(ITERS):
        current = advance(with_rim(current), east_rim, north_rim, diffusivity_rim, seawater_rim)
    return reorder(current[:, 0], dynamics_blocks)
```

```python
import jax
import jax.numpy as jnp
from jax import lax
from jax.experimental import pallas as pl
from jax.experimental.pallas import tpu as pltpu
from jax.sharding import PartitionSpec as P

K = 8
BR = 8
ITERS = 4
HALO = ITERS + 1
LANES = 128
SLOTS = 3
GROUPS = 3
VREGS = 6

TIME_STEP = 0.2
STRATIFICATION = 1.0
DENSITY_FLOOR = 0.25
SLOPE_LIMIT = 1.0
TAPER_WIDTH = 0.5
KERNEL_OFFSET = 0.05
BASE_DIFFUSIVITY = 0.2
VISBECK_ALPHA = 0.5


def rolled(x, shift):
    shift %= LANES
    return x if shift == 0 else pltpu.roll(x, shift, x.ndim - 1)


def lane_of(shape=(BR, LANES)):
    return lax.broadcasted_iota(jnp.int32, shape, len(shape) - 1)


def plane_at(register, piece):
    if piece == 2 and register == 2:
        return 2 * K
    if piece == 2 and register == 5:
        return 2 * K + 1
    return register % 3 + 3 * piece + (K if register >= 3 else 0)


def edges_kernel(d_first, d_last, t_first, t_last, s_first, s_last, m_first, m_last, head_ref, tail_ref):
    shape = (d_first.shape[1], LANES)
    lane = lane_of(shape)

    def gather(density, tracer, mask, mixed, start):
        out = jnp.zeros(shape, jnp.float32)
        for p in range(2 * K + 2):
            if p < K:
                plane = density[p]
            elif p < 2 * K:
                plane = tracer[p - K]
            else:
                plane = (mask if p == 2 * K else mixed)[...].astype(jnp.float32)
            at = HALO * p
            out = jnp.where((lane >= at) & (lane < at + HALO), rolled(plane, at - start), out)
        return out

    head_ref[...] = gather(d_first, t_first, s_first, m_first, 0)
    tail_ref[...] = gather(d_last, t_last, s_last, m_last, LANES - HALO)


def edges(density, tracer, mask, mixed):
    rows, columns = mask.shape
    last = columns // LANES - 1
    cube = lambda c: pl.BlockSpec((K, rows, LANES), lambda i: (0, 0, c))
    flat = lambda c: pl.BlockSpec((rows, LANES), lambda i: (0, c))
    out = jax.ShapeDtypeStruct((rows, LANES), jnp.float32)
    rim = pl.BlockSpec((rows, LANES), lambda i: (0, 0))
    return pl.pallas_call(
        edges_kernel,
        grid=(1,),
        out_shape=(out, out),
        out_specs=(rim, rim),
        in_specs=[cube(0), cube(last), cube(0), cube(last), flat(0), flat(last), flat(0), flat(last)],
        name="edges",
    )(density, density, tracer, tracer, mask, mask, mixed, mixed)


def pack_kernel(width, density, tracer, mask, mixed, out_ref):
    piece = width + 2 * HALO
    per_tile = LANES // width
    tiles = mask.shape[1] // LANES
    lane = lane_of()

    def columns(p):
        for t in range(tiles):
            at = slice(LANES * t, LANES * (t + 1))
            if p < K:
                yield density[p, :, at]
            elif p < 2 * K:
                yield tracer[p - K, :, at]
            else:
                yield (mask if p == 2 * K else mixed)[:, at].astype(jnp.float32)

    for v in range(VREGS):
        whole, seam = [], []
        for m in range(SLOTS):
            own = list(columns(plane_at(v, m)))
            whole.append(own)
            seam.append(
                [own[0]]
                + [jnp.where(lane < LANES // 2, own[t], own[t - 1]) for t in range(1, tiles)]
                + [own[-1]]
            )
        for j in range(tiles * per_tile):
            t, q = divmod(j, per_tile)
            parts = []
            for m in range(SLOTS):
                if q == 0:
                    source = seam[m][t]
                elif q == per_tile - 1:
                    source = seam[m][t + 1]
                else:
                    source = whole[m][t]
                parts.append(rolled(source, piece * m - (width * q - HALO)))
            out_ref[j, v] = jnp.where(
                lane < piece, parts[0], jnp.where(lane < 2 * piece, parts[1], parts[2])
            )


def pack(density, tracer, mask, mixed, strips):
    rows, columns = mask.shape
    blocks = rows // BR
    width = columns // strips
    cube = pl.BlockSpec((K, BR, columns), lambda b: (0, b, 0))
    flat = pl.BlockSpec((BR, columns), lambda b: (b, 0))

    def kernel(*refs):
        pack_kernel(width, *refs)

    return pl.pallas_call(
        kernel,
        grid=(blocks,),
        out_shape=jax.ShapeDtypeStruct((strips, blocks * VREGS, BR, LANES), jnp.float32),
        in_specs=[cube, cube, flat, flat],
        out_specs=pl.BlockSpec((strips, VREGS, BR, LANES), lambda b: (0, b, 0, 0)),
        cost_estimate=pl.CostEstimate(flops=20000000, bytes_accessed=6000000, transcendentals=0),
        name="pack",
    )(density, tracer, mask, mixed)


def patch_kernel(piece, west, east, packed, out_ref):
    lane = lane_of()
    blocks = west.shape[0] // BR

    def fill(edge, start):
        for b in range(blocks):
            rim = edge[BR * b : BR * (b + 1), :]
            for v in range(VREGS):
                value = packed[0, b * VREGS + v]
                for m in range(SLOTS):
                    at = piece * m + start
                    here = (lane >= at) & (lane < at + HALO)
                    value = jnp.where(here, rolled(rim, at - HALO * plane_at(v, m)), value)
                out_ref[0, b * VREGS + v] = value

    pl.when(pl.program_id(0) == 0)(lambda: fill(west, 0))
    pl.when(pl.program_id(0) == 1)(lambda: fill(east, piece - HALO))


def patch(west, east, packed, piece):
    strips, count = packed.shape[:2]
    rim = pl.BlockSpec(west.shape, lambda i: (0, 0))
    ends = pl.BlockSpec((1, count, BR, LANES), lambda i: (i * (strips - 1), 0, 0, 0))

    def kernel(*refs):
        patch_kernel(piece, *refs)

    return pl.pallas_call(
        kernel,
        grid=(2,),
        out_shape=jax.ShapeDtypeStruct(packed.shape, jnp.float32),
        in_specs=[rim, rim, ends],
        out_specs=ends,
        input_output_aliases={2: 0},
        name="patch",
    )(west, east, packed)


def sweep_kernel(
    width, blocks, order, owner, got, out_ref, slot_of, rho, sea, ta, tb, cp, cq, cr, kap, ce, cw, cn, me, mw
):
    piece = width + 2 * HALO
    lane = lane_of()
    first = lane < piece
    second = lane < 2 * piece
    slot = jnp.where(first, 0, jnp.where(second, 1, 2))
    zeros = jnp.zeros((BR, LANES), jnp.float32)

    def invert(s, carry):
        slot_of[order[s]] = s
        return carry

    lax.fori_loop(0, blocks, invert, 0)

    for edge in (0, BR * (blocks + 1)):
        for g in range(GROUPS):
            rho[g, pl.ds(edge, BR), :] = zeros
            ta[g, pl.ds(edge, BR), :] = zeros
            tb[g, pl.ds(edge, BR), :] = zeros
        sea[pl.ds(edge, BR), :] = zeros
        kap[pl.ds(edge, BR), :] = zeros
        cn[pl.ds(edge, BR), :] = zeros

    def spread(x):
        return jnp.where(first, rolled(x, -2 * piece), jnp.where(second, rolled(x, -piece), x))

    def loop(body, step=1):
        def some(i, carry):
            for u in range(step):
                body(i * step + u)
            return carry

        lax.fori_loop(0, blocks // step, some, 0)

    def rows(b, off=0):
        if off == 0:
            return pl.ds(pl.multiple_of(BR * (b + 1), BR), BR)
        return pl.ds(BR * (b + 1) + off, BR)

    def gather(b):
        s = slot_of[b]
        t = owner[s]
        for g in range(GROUPS):
            rho[g, rows(b), :] = got[s, g]
            ta[g, rows(b), :] = got[t, GROUPS + g]
        sea[rows(b), :] = spread(got[s, 2])

    loop(gather, 2)

    def deltas(f):
        f0, f1, f2 = f
        f2 = jnp.where(second, f2, f1)
        above0 = jnp.where(first, f0, rolled(f2, piece))
        return (f1 - above0, f2 - f0, rolled(f0, -piece) - f1)

    def physics(b):
        s = slot_of[b]
        mixed = spread(got[s, 5])
        here = sea[rows(b), :]
        north = sea[rows(b, 1), :] * here
        south = sea[rows(b, -1), :] * here
        east = rolled(here, -1) * here
        west = rolled(east, 1)
        me[rows(b), :] = east
        mw[rows(b), :] = west
        f = [rho[g, rows(b), :] for g in range(GROUPS)]
        down = deltas(f)
        per_mixed = 1.0 / (mixed + 1.0)
        total = zeros
        kept = []
        for g in range(GROUPS):
            level = (slot * 3 + g).astype(jnp.float32)
            step = rolled(f[g], -1) - f[g]
            sum_e = east * step + west * rolled(step, 1)
            sum_n = north * (rho[g, rows(b, 1), :] - f[g]) + south * (f[g] - rho[g, rows(b, -1), :])
            rising = jnp.where((level == 0.0) | (level == K - 1.0), 0.5 * STRATIFICATION, STRATIFICATION)
            denominator = jnp.maximum(0.5 * down[g] + rising, DENSITY_FLOOR)
            scale = -0.5 / denominator
            se = sum_e * scale
            sn = sum_n * scale
            squared = se * se + sn * sn
            taper = 0.5 + 0.5 * jnp.tanh((SLOPE_LIMIT - squared) * (1.0 / TAPER_WIDTH))
            factor = taper * jnp.minimum(1.0, (level + 1.0) * per_mixed) * here
            se = se * factor
            sn = sn * factor
            squared = se * se + sn * sn
            below = (level >= mixed) & (level < K)
            total += jnp.where(below, jnp.sqrt(denominator * (squared + KERNEL_OFFSET)), 0.0)
            kept.append((se, sn, squared))
        total = total + rolled(total, -piece) + rolled(total, -2 * piece)
        total = jnp.where(first, total, jnp.where(second, rolled(total, piece), rolled(total, 2 * piece)))
        kappa = here * (BASE_DIFFUSIVITY + VISBECK_ALPHA * total / (K - mixed))
        kap[rows(b), :] = kappa
        weight = (0.5 * TIME_STEP) * kappa
        for g in range(GROUPS):
            se, sn, squared = kept[g]
            w = jnp.where(second, weight, 0.0) if g == 2 else weight
            cp[g, rows(b), :] = w * se
            cq[g, rows(b), :] = w * sn
            cr[g, rows(b), :] = (0.5 * w) * squared

    loop(physics)

    def faces(b):
        kappa = kap[rows(b), :]
        here = sea[rows(b), :]
        east = (0.5 * TIME_STEP) * (kappa + rolled(kappa, -1)) * me[rows(b), :]
        ce[rows(b), :] = east
        cw[rows(b), :] = rolled(east, 1)
        cn[rows(b), :] = (0.5 * TIME_STEP) * (kappa + kap[rows(b, 1), :]) * (here * sea[rows(b, 1), :])

    loop(faces, 2)

    def advance(b, source):
        here = sea[rows(b), :]
        north = sea[rows(b, 1), :] * here
        south = sea[rows(b, -1), :] * here
        east = me[rows(b), :]
        west = mw[rows(b), :]
        face_e = ce[rows(b), :]
        face_w = cw[rows(b), :]
        face_n = cn[rows(b), :]
        face_s = cn[rows(b, -1), :]
        f = [source[g, rows(b), :] for g in range(GROUPS)]
        down = deltas(f)
        flux, result = [], []
        for g in range(GROUPS):
            step_e = rolled(f[g], -1) - f[g]
            step_w = rolled(step_e, 1)
            step_n = source[g, rows(b, 1), :] - f[g]
            step_s = f[g] - source[g, rows(b, -1), :]
            sum_e = east * step_e + west * step_w
            sum_n = north * step_n + south * step_s
            lateral = (face_e * step_e - face_w * step_w) + (face_n * step_n - face_s * step_s)
            flux.append(
                cp[g, rows(b), :] * sum_e + cq[g, rows(b), :] * sum_n + cr[g, rows(b), :] * down[g]
            )
            result.append(f[g] + lateral)
        result[0] += flux[1] - rolled(flux[2], piece)
        result[1] += flux[2] - flux[0]
        result[2] += rolled(flux[0], -piece) - flux[1]
        return result

    def sweep(source, target):
        def body(b):
            result = advance(b, source)
            for g in range(GROUPS):
                target[g, rows(b), :] = result[g]

        loop(body)

    sweep(ta, tb)
    sweep(tb, ta)
    sweep(ta, tb)

    per_out = LANES // width

    def last(b):
        result = advance(b, tb)
        t = owner[slot_of[b]]
        for h in range(K // per_out):
            value = None
            for m in range(per_out):
                k = h * per_out + m
                part = rolled(result[k % 3], width * m - (piece * (k // 3) + HALO))
                value = part if m == 0 else jnp.where(lane < width * m, value, part)
            out_ref[t, h] = value

    loop(last)


def sweeps(order, owner, got, width):
    blocks = got.shape[0]
    padded = BR * (blocks + 2)
    cube = pltpu.VMEM((GROUPS, padded, LANES), jnp.float32)
    flat = pltpu.VMEM((padded, LANES), jnp.float32)
    outs = K * width // LANES

    def kernel(*refs):
        sweep_kernel(width, blocks, *refs)

    return pl.pallas_call(
        kernel,
        out_shape=jax.ShapeDtypeStruct((blocks, outs, BR, LANES), jnp.float32),
        in_specs=[
            pl.BlockSpec(memory_space=pltpu.SMEM),
            pl.BlockSpec(memory_space=pltpu.SMEM),
            pl.BlockSpec(memory_space=pltpu.VMEM),
        ],
        out_specs=pl.BlockSpec(memory_space=pltpu.VMEM),
        scratch_shapes=[pltpu.SMEM((blocks,), jnp.int32), cube, flat]
        + [cube] * 5
        + [flat] * 6,
        compiler_params=pltpu.CompilerParams(vmem_limit_bytes=40 * 1024 * 1024),
        name="sweeps",
    )(order, owner, got)


def unpack_kernel(width, got, out_ref):
    per_tile = LANES // width
    tiles = out_ref.shape[2] // LANES
    lane = lane_of()
    for k in range(K):
        h, m = divmod(k, per_tile)
        for t in range(tiles):
            value = None
            for q in range(per_tile):
                part = rolled(got[t * per_tile + q, h], width * (q - m))
                value = part if q == 0 else jnp.where(lane < width * q, value, part)
            out_ref[k, :, LANES * t : LANES * (t + 1)] = value


def unpack(got, rows, columns):
    strips = got.shape[0]
    blocks = rows // BR
    width = columns // strips
    outs = K * width // LANES

    def kernel(*refs):
        unpack_kernel(width, *refs)

    return pl.pallas_call(
        kernel,
        grid=(blocks,),
        out_shape=jax.ShapeDtypeStruct((K, rows, columns), jnp.float32),
        in_specs=[pl.BlockSpec((strips, outs, BR, LANES), lambda b: (0, b, 0, 0))],
        out_specs=pl.BlockSpec((K, BR, columns), lambda b: (0, b, 0)),
        name="unpack",
    )(got)


def on_device(density, tracer, sea_mask, mixed_level, tile_blocks, block_owner):
    rows, columns = sea_mask.shape
    strips = lax.axis_size("gy")
    ring = lax.axis_size("gx")
    width = columns // strips
    blocks = rows // BR
    head, tail = edges(density, tracer, sea_mask, mixed_level)
    west = lax.ppermute(tail, "gx", [(i, (i + 1) % ring) for i in range(ring)])
    east = lax.ppermute(head, "gx", [((i + 1) % ring, i) for i in range(ring)])
    packed = pack(density, tracer, sea_mask, mixed_level, strips)
    packed = patch(west, east, packed, width + 2 * HALO)
    got = lax.all_to_all(packed, "gy", split_axis=0, concat_axis=0, tiled=True)
    done = sweeps(tile_blocks, block_owner, got.reshape(strips * blocks, VREGS, BR, LANES), width)
    back = lax.all_to_all(
        done.reshape(strips, -1, BR, LANES), "gy", split_axis=0, concat_axis=0, tiled=True
    )
    return unpack(back, rows, columns)


def solution(mesh):
    placed = (P(None, "gy", "gx"), P(None, "gy", "gx"), P("gy", "gx"), P("gy", "gx"), P(), P())
    return jax.shard_map(
        on_device, mesh=mesh, in_specs=placed, out_specs=P(None, "gy", "gx"), check_vma=False
    )
```

```python
import jax
import jax.numpy as jnp
from jax import lax
from jax.experimental import pallas as pl
from jax.experimental.pallas import tpu as pltpu
from jax.sharding import PartitionSpec as P

K = 8
BR = 8
ITERS = 4
HALO = ITERS + 1
LANES = 128
SLOTS = 3
VREGS = 6
UNIT = 4
GATHER = 4
PHYSICS = 2
FACES = 4
SWEEP = 4
LAST = 4

TIME_STEP = 0.2
STRATIFICATION = 1.0
DENSITY_FLOOR = 0.25
SLOPE_LIMIT = 1.0
TAPER_WIDTH = 0.5
KERNEL_OFFSET = 0.05
BASE_DIFFUSIVITY = 0.2
VISBECK_ALPHA = 0.5


def rolled(x, shift):
    shift %= LANES
    return x if shift == 0 else pltpu.roll(x, shift, x.ndim - 1)


def lane_of(shape=(BR, LANES)):
    return lax.broadcasted_iota(jnp.int32, shape, len(shape) - 1)


def plane_at(register, piece):
    if piece == 2 and register == 2:
        return 2 * K
    if piece == 2 and register == 5:
        return 2 * K + 1
    return register % 3 + 3 * piece + (K if register >= 3 else 0)


def edges_kernel(d_first, d_last, t_first, t_last, s_first, s_last, m_first, m_last, head_ref, tail_ref):
    shape = (d_first.shape[1], LANES)
    lane = lane_of(shape)

    def gather(density, tracer, mask, mixed, start):
        out = jnp.zeros(shape, jnp.float32)
        for p in range(2 * K + 2):
            if p < K:
                plane = density[p]
            elif p < 2 * K:
                plane = tracer[p - K]
            else:
                plane = (mask if p == 2 * K else mixed)[...].astype(jnp.float32)
            at = HALO * p
            out = jnp.where((lane >= at) & (lane < at + HALO), rolled(plane, at - start), out)
        return out

    head_ref[...] = gather(d_first, t_first, s_first, m_first, 0)
    tail_ref[...] = gather(d_last, t_last, s_last, m_last, LANES - HALO)


def edges(density, tracer, mask, mixed):
    rows, columns = mask.shape
    last = columns // LANES - 1
    cube = lambda c: pl.BlockSpec((K, rows, LANES), lambda i: (0, 0, c))
    flat = lambda c: pl.BlockSpec((rows, LANES), lambda i: (0, c))
    out = jax.ShapeDtypeStruct((rows, LANES), jnp.float32)
    rim = pl.BlockSpec((rows, LANES), lambda i: (0, 0))
    return pl.pallas_call(
        edges_kernel,
        grid=(1,),
        out_shape=(out, out),
        out_specs=(rim, rim),
        in_specs=[cube(0), cube(last), cube(0), cube(last), flat(0), flat(last), flat(0), flat(last)],
        name="edges",
    )(density, density, tracer, tracer, mask, mask, mixed, mixed)


def pack_kernel(width, density, tracer, mask, mixed, out_ref):
    piece = width + 2 * HALO
    per_tile = LANES // width
    tiles = mask.shape[1] // LANES
    lane = lane_of()

    def columns(p):
        for t in range(tiles):
            at = slice(LANES * t, LANES * (t + 1))
            if p < K:
                yield density[p, :, at]
            elif p < 2 * K:
                yield tracer[p - K, :, at]
            else:
                yield (mask if p == 2 * K else mixed)[:, at].astype(jnp.float32)

    for v in range(VREGS):
        whole, seam = [], []
        for m in range(SLOTS):
            own = list(columns(plane_at(v, m)))
            whole.append(own)
            seam.append(
                [own[0]]
                + [jnp.where(lane < LANES // 2, own[t], own[t - 1]) for t in range(1, tiles)]
                + [own[-1]]
            )
        for j in range(tiles * per_tile):
            t, q = divmod(j, per_tile)
            parts = []
            for m in range(SLOTS):
                if q == 0:
                    source = seam[m][t]
                elif q == per_tile - 1:
                    source = seam[m][t + 1]
                else:
                    source = whole[m][t]
                parts.append(rolled(source, piece * m - (width * q - HALO)))
            out_ref[j, v] = jnp.where(
                lane < piece, parts[0], jnp.where(lane < 2 * piece, parts[1], parts[2])
            )


def pack(density, tracer, mask, mixed, strips):
    rows, columns = mask.shape
    blocks = rows // BR
    width = columns // strips
    cube = pl.BlockSpec((K, BR, columns), lambda b: (0, b, 0))
    flat = pl.BlockSpec((BR, columns), lambda b: (b, 0))

    def kernel(*refs):
        pack_kernel(width, *refs)

    return pl.pallas_call(
        kernel,
        grid=(blocks,),
        out_shape=jax.ShapeDtypeStruct((strips, blocks * VREGS, BR, LANES), jnp.float32),
        in_specs=[cube, cube, flat, flat],
        out_specs=pl.BlockSpec((strips, VREGS, BR, LANES), lambda b: (0, b, 0, 0)),
        cost_estimate=pl.CostEstimate(flops=20000000, bytes_accessed=6000000, transcendentals=0),
        name="pack",
    )(density, tracer, mask, mixed)


def patch_kernel(piece, west, east, packed, out_ref):
    lane = lane_of()
    blocks = west.shape[0] // BR

    def fill(edge, start):
        for b in range(blocks):
            rim = edge[BR * b : BR * (b + 1), :]
            for v in range(VREGS):
                value = packed[0, b * VREGS + v]
                for m in range(SLOTS):
                    at = piece * m + start
                    here = (lane >= at) & (lane < at + HALO)
                    value = jnp.where(here, rolled(rim, at - HALO * plane_at(v, m)), value)
                out_ref[0, b * VREGS + v] = value

    pl.when(pl.program_id(0) == 0)(lambda: fill(west, 0))
    pl.when(pl.program_id(0) == 1)(lambda: fill(east, piece - HALO))


def patch(west, east, packed, piece):
    strips, count = packed.shape[:2]
    rim = pl.BlockSpec(west.shape, lambda i: (0, 0))
    ends = pl.BlockSpec((1, count, BR, LANES), lambda i: (i * (strips - 1), 0, 0, 0))

    def kernel(*refs):
        patch_kernel(piece, *refs)

    return pl.pallas_call(
        kernel,
        grid=(2,),
        out_shape=jax.ShapeDtypeStruct(packed.shape, jnp.float32),
        in_specs=[rim, rim, ends],
        out_specs=ends,
        input_output_aliases={2: 0},
        name="patch",
    )(west, east, packed)


def sweep_kernel(
    width, blocks, order, owner, got, out_ref, slot_of, rho, ta, tb, cp, cq, cr, sea, mix, kap, me, mw, mn, ms, ce, cw, cn, cs
):
    piece = width + 2 * HALO
    depth = (sea.shape[0] - 2 * BR) // BR
    lane = lane_of()
    first = lane < piece
    second = lane < 2 * piece

    def invert(s, carry):
        slot_of[order[s]] = s
        return carry

    lax.fori_loop(0, blocks, invert, 0)
    for b in range(blocks, SLOTS * depth):
        slot_of[b] = slot_of[0]

    def loop(body, count, chunk):
        def some(i, carry):
            body(i)
            return carry

        lax.fori_loop(0, count // chunk, some, 0)

    def rows(c, off=0, chunk=1):
        start = BR + BR * chunk * c
        if off == 0:
            return pl.ds(pl.multiple_of(start, BR), BR * chunk)
        return pl.ds(start + off, BR * chunk)

    def close(ref):
        top = jnp.where(first, 0.0, rolled(ref[pl.ds(BR * depth, BR), :], piece))
        bottom = jnp.where(second, rolled(ref[pl.ds(BR, BR), :], -piece), 0.0)
        ref[pl.ds(0, BR), :] = top
        ref[pl.ds(BR * (depth + 1), BR), :] = bottom

    def gather(c):
        for u in range(GATHER):
            i = c * GATHER + u
            slots = [slot_of[i + depth * m] for m in range(SLOTS)]
            owners = [owner[s] for s in slots]
            real = jnp.where(i + depth * (SLOTS - 1) < blocks, 1.0, 0.0)

            def plane(v, n, where):
                parts = [rolled(got[where[m], v], piece * (m - n)) for m in range(SLOTS)]
                return jnp.where(first, parts[0], jnp.where(second, parts[1], parts[2] * real))

            at = rows(i)
            for k in range(K):
                rho[k, at, :] = plane(k % 3, k // 3, slots)
                ta[k, at, :] = plane(3 + k % 3, k // 3, owners)
            sea[at, :] = plane(2, 2, slots)
            mix[at, :] = plane(5, 2, slots)

    loop(gather, depth, GATHER)
    for k in range(K):
        close(rho.at[k])
        close(ta.at[k])
    close(sea)

    def physics(c):
        at, up, down = (rows(c, off, PHYSICS) for off in (0, 1, -1))
        mixed = mix[at, :]
        here = sea[at, :]
        east = rolled(here, -1) * here
        west = rolled(here, 1) * here
        north = sea[up, :] * here
        south = sea[down, :] * here
        me[at, :] = east
        mw[at, :] = west
        mn[at, :] = north
        ms[at, :] = south
        per_mixed = 1.0 / (mixed + 1.0)
        f = [rho[k, at, :] for k in range(K)]
        total = jnp.zeros_like(here)
        kept = []
        for k in range(K):
            sum_e = east * (rolled(f[k], -1) - f[k]) + west * (f[k] - rolled(f[k], 1))
            sum_n = north * (rho[k, up, :] - f[k]) + south * (f[k] - rho[k, down, :])
            above, under = max(k - 1, 0), min(k + 1, K - 1)
            rising = 0.5 * STRATIFICATION * (under - above)
            denominator = jnp.maximum(0.5 * (f[under] - f[above]) + rising, DENSITY_FLOOR)
            scale = -0.5 / denominator
            se = sum_e * scale
            sn = sum_n * scale
            squared = se * se + sn * sn
            taper = 0.5 + 0.5 * jnp.tanh((SLOPE_LIMIT - squared) * (1.0 / TAPER_WIDTH))
            factor = taper * jnp.minimum(1.0, (k + 1.0) * per_mixed) * here
            se = se * factor
            sn = sn * factor
            squared = se * se + sn * sn
            root = jnp.sqrt(denominator * (squared + KERNEL_OFFSET))
            total += jnp.where(mixed <= float(k), root, 0.0)
            cp[k, at, :] = se
            cq[k, at, :] = sn
            kept.append(squared)
        kappa = here * (BASE_DIFFUSIVITY + VISBECK_ALPHA * total / (K - mixed))
        kap[at, :] = kappa
        weight = (0.5 * TIME_STEP) * kappa
        for k in range(K):
            cp[k, at, :] = weight * cp[k, at, :]
            cq[k, at, :] = weight * cq[k, at, :]
            cr[k, at, :] = (0.5 * weight) * kept[k]

    loop(physics, depth, PHYSICS)
    close(kap)

    def faces(c):
        at, up, down = (rows(c, off, FACES) for off in (0, 1, -1))
        kappa = (0.5 * TIME_STEP) * kap[at, :]
        ce[at, :] = (kappa + rolled(kappa, -1)) * me[at, :]
        cw[at, :] = (kappa + rolled(kappa, 1)) * mw[at, :]
        cn[at, :] = (kappa + (0.5 * TIME_STEP) * kap[up, :]) * mn[at, :]
        cs[at, :] = (kappa + (0.5 * TIME_STEP) * kap[down, :]) * ms[at, :]

    loop(faces, depth, FACES)

    def advance(c, source, chunk):
        at, up, down = (rows(c, off, chunk) for off in (0, 1, -1))
        mask_e, mask_w, mask_n, mask_s = (ref[at, :] for ref in (me, mw, mn, ms))
        face_e, face_w, face_n, face_s = (ref[at, :] for ref in (ce, cw, cn, cs))
        f = [source[k, at, :] for k in range(K)]
        flux, result = [], []
        for k in range(K):
            step_e = rolled(f[k], -1) - f[k]
            step_w = f[k] - rolled(f[k], 1)
            step_n = source[k, up, :] - f[k]
            step_s = f[k] - source[k, down, :]
            sum_e = mask_e * step_e + mask_w * step_w
            sum_n = mask_n * step_n + mask_s * step_s
            lateral = (face_e * step_e - face_w * step_w) + (face_n * step_n - face_s * step_s)
            drop = f[min(k + 1, K - 1)] - f[max(k - 1, 0)]
            flux.append(cp[k, at, :] * sum_e + cq[k, at, :] * sum_n + cr[k, at, :] * drop)
            result.append(f[k] + lateral)
        for k in range(K):
            if k + 1 < K:
                result[k] += flux[k + 1]
            if k > 0:
                result[k] -= flux[k - 1]
        return result

    def sweep(source, target):
        def body(c):
            result = advance(c, source, SWEEP)
            for k in range(K):
                target[k, rows(c, 0, SWEEP), :] = result[k]

        loop(body, depth, SWEEP)
        for k in range(K):
            close(target.at[k])

    for n in range(ITERS - 1):
        sweep(*((ta, tb) if n % 2 == 0 else (tb, ta)))
    source = ta if (ITERS - 1) % 2 == 0 else tb
    per_out = LANES // width
    wide = lane_of((BR * LAST, LANES))

    def last(back):
        c = depth // LAST - 1 - back
        result = advance(c, source, LAST)
        for g in reversed(range(SLOTS)):
            for h in range(K // per_out):
                value = None
                for m in range(per_out):
                    part = rolled(result[h * per_out + m], width * m - (piece * g + HALO))
                    value = part if m == 0 else jnp.where(wide < width * m, value, part)
                for u in range(LAST):
                    t = owner[slot_of[c * LAST + u + depth * g]]
                    out_ref[t, h] = value[BR * u : BR * (u + 1), :]

    loop(last, depth, LAST)


def sweeps(order, owner, got, width):
    blocks = got.shape[0]
    depth = -(-blocks // (SLOTS * UNIT)) * UNIT
    padded = BR * (depth + 2)
    cube = pltpu.VMEM((K, padded, LANES), jnp.float32)
    flat = pltpu.VMEM((padded, LANES), jnp.float32)
    outs = K * width // LANES

    def kernel(*refs):
        sweep_kernel(width, blocks, *refs)

    return pl.pallas_call(
        kernel,
        out_shape=jax.ShapeDtypeStruct((blocks, outs, BR, LANES), jnp.float32),
        in_specs=[
            pl.BlockSpec(memory_space=pltpu.SMEM),
            pl.BlockSpec(memory_space=pltpu.SMEM),
            pl.BlockSpec(memory_space=pltpu.VMEM),
        ],
        out_specs=pl.BlockSpec(memory_space=pltpu.VMEM),
        scratch_shapes=[pltpu.SMEM((SLOTS * depth,), jnp.int32)] + [cube] * 6 + [flat] * 11,
        compiler_params=pltpu.CompilerParams(vmem_limit_bytes=40 * 1024 * 1024),
        name="sweeps",
    )(order, owner, got)


def unpack_kernel(width, got, out_ref):
    per_tile = LANES // width
    tiles = out_ref.shape[2] // LANES
    lane = lane_of()
    for k in range(K):
        h, m = divmod(k, per_tile)
        for t in range(tiles):
            value = None
            for q in range(per_tile):
                part = rolled(got[t * per_tile + q, h], width * (q - m))
                value = part if q == 0 else jnp.where(lane < width * q, value, part)
            out_ref[k, :, LANES * t : LANES * (t + 1)] = value


def unpack(got, rows, columns):
    strips = got.shape[0]
    blocks = rows // BR
    width = columns // strips
    outs = K * width // LANES

    def kernel(*refs):
        unpack_kernel(width, *refs)

    return pl.pallas_call(
        kernel,
        grid=(blocks,),
        out_shape=jax.ShapeDtypeStruct((K, rows, columns), jnp.float32),
        in_specs=[pl.BlockSpec((strips, outs, BR, LANES), lambda b: (0, b, 0, 0))],
        out_specs=pl.BlockSpec((K, BR, columns), lambda b: (0, b, 0)),
        name="unpack",
    )(got)


def on_device(density, tracer, sea_mask, mixed_level, tile_blocks, block_owner):
    rows, columns = sea_mask.shape
    strips = lax.axis_size("gy")
    ring = lax.axis_size("gx")
    width = columns // strips
    blocks = rows // BR
    head, tail = edges(density, tracer, sea_mask, mixed_level)
    west = lax.ppermute(tail, "gx", [(i, (i + 1) % ring) for i in range(ring)])
    east = lax.ppermute(head, "gx", [((i + 1) % ring, i) for i in range(ring)])
    packed = pack(density, tracer, sea_mask, mixed_level, strips)
    packed = patch(west, east, packed, width + 2 * HALO)
    got = lax.all_to_all(packed, "gy", split_axis=0, concat_axis=0, tiled=True)
    done = sweeps(tile_blocks, block_owner, got.reshape(strips * blocks, VREGS, BR, LANES), width)
    back = lax.all_to_all(
        done.reshape(strips, -1, BR, LANES), "gy", split_axis=0, concat_axis=0, tiled=True
    )
    return unpack(back, rows, columns)


def solution(mesh):
    placed = (P(None, "gy", "gx"), P(None, "gy", "gx"), P("gy", "gx"), P("gy", "gx"), P(), P())
    return jax.shard_map(
        on_device, mesh=mesh, in_specs=placed, out_specs=P(None, "gy", "gx"), check_vma=False
    )
```

```python
import jax
import jax.numpy as jnp
from jax import lax
from jax.experimental import pallas as pl
from jax.experimental.pallas import tpu as pltpu
from jax.sharding import PartitionSpec as P

K = 8
BR = 8
ITERS = 4
HALO = ITERS + 1
LANES = 128
SLOTS = 3
VREGS = 6
PACK = 2
UNPACK = 2
SMALL = 12 * 1024 * 1024
UNIT = 4
GATHER = 11
PHYSICS = 4
FACES = 4
SWEEP = 4
LAST = 4

TIME_STEP = 0.2
STRATIFICATION = 1.0
DENSITY_FLOOR = 0.25
SLOPE_LIMIT = 1.0
TAPER_WIDTH = 0.5
KERNEL_OFFSET = 0.05
BASE_DIFFUSIVITY = 0.2
VISBECK_ALPHA = 0.5


def rolled(x, shift):
    shift %= LANES
    return x if shift == 0 else pltpu.roll(x, shift, x.ndim - 1)


def lane_of(shape=(BR, LANES)):
    return lax.broadcasted_iota(jnp.int32, shape, len(shape) - 1)


def plane_at(register, piece):
    if piece == 2 and register == 2:
        return 2 * K
    if piece == 2 and register == 5:
        return 2 * K + 1
    return register % 3 + 3 * piece + (K if register >= 3 else 0)


def edges_kernel(d_first, d_last, t_first, t_last, s_first, s_last, m_first, m_last, head_ref, tail_ref):
    shape = (d_first.shape[1], LANES)
    lane = lane_of(shape)

    def gather(density, tracer, mask, mixed, start):
        out = jnp.zeros(shape, jnp.float32)
        for p in range(2 * K + 2):
            if p < K:
                plane = density[p]
            elif p < 2 * K:
                plane = tracer[p - K]
            else:
                plane = (mask if p == 2 * K else mixed)[...].astype(jnp.float32)
            at = HALO * p
            out = jnp.where((lane >= at) & (lane < at + HALO), rolled(plane, at - start), out)
        return out

    head_ref[...] = gather(d_first, t_first, s_first, m_first, 0)
    tail_ref[...] = gather(d_last, t_last, s_last, m_last, LANES - HALO)


def edges(density, tracer, mask, mixed):
    rows, columns = mask.shape
    last = columns // LANES - 1
    cube = lambda c: pl.BlockSpec((K, rows, LANES), lambda i: (0, 0, c))
    flat = lambda c: pl.BlockSpec((rows, LANES), lambda i: (0, c))
    out = jax.ShapeDtypeStruct((rows, LANES), jnp.float32)
    rim = pl.BlockSpec((rows, LANES), lambda i: (0, 0))
    return pl.pallas_call(
        edges_kernel,
        grid=(1,),
        out_shape=(out, out),
        out_specs=(rim, rim),
        compiler_params=pltpu.CompilerParams(vmem_limit_bytes=SMALL),
        in_specs=[cube(0), cube(last), cube(0), cube(last), flat(0), flat(last), flat(0), flat(last)],
        name="edges",
    )(density, density, tracer, tracer, mask, mask, mixed, mixed)


def pack_kernel(width, density, tracer, mask, mixed, out_ref):
    piece = width + 2 * HALO
    per_tile = LANES // width
    tiles = mask.shape[1] // LANES
    count = mask.shape[0] // BR
    lane = lane_of()

    def columns(p, row):
        for t in range(tiles):
            at = slice(LANES * t, LANES * (t + 1))
            if p < K:
                yield density[p, row, at]
            elif p < 2 * K:
                yield tracer[p - K, row, at]
            else:
                yield (mask if p == 2 * K else mixed)[row, at].astype(jnp.float32)

    for u in range(count):
        block = pl.program_id(0) * count + u
        for v in range(VREGS):
            whole, seam = [], []
            for m in range(SLOTS):
                own = list(columns(plane_at(v, m), slice(BR * u, BR * (u + 1))))
                whole.append(own)
                seam.append(
                    [own[0]]
                    + [jnp.where(lane < LANES // 2, own[t], own[t - 1]) for t in range(1, tiles)]
                    + [own[-1]]
                )
            for j in range(tiles * per_tile):
                t, q = divmod(j, per_tile)
                parts = []
                for m in range(SLOTS):
                    if q == 0:
                        source = seam[m][t]
                    elif q == per_tile - 1:
                        source = seam[m][t + 1]
                    else:
                        source = whole[m][t]
                    parts.append(rolled(source, piece * m - (width * q - HALO)))
                out_ref[j, block * VREGS + v] = jnp.where(
                    lane < piece, parts[0], jnp.where(lane < 2 * piece, parts[1], parts[2])
                )


def pack(density, tracer, mask, mixed, strips):
    rows, columns = mask.shape
    blocks = rows // BR
    width = columns // strips
    tall = rows // PACK
    cube = pl.BlockSpec((K, tall, columns), lambda b: (0, b, 0))
    flat = pl.BlockSpec((tall, columns), lambda b: (b, 0))

    def kernel(*refs):
        pack_kernel(width, *refs)

    return pl.pallas_call(
        kernel,
        grid=(PACK,),
        out_shape=jax.ShapeDtypeStruct((strips, blocks * VREGS, BR, LANES), jnp.float32),
        in_specs=[cube, cube, flat, flat],
        out_specs=pl.BlockSpec(memory_space=pltpu.VMEM),
        compiler_params=pltpu.CompilerParams(vmem_limit_bytes=SMALL),
        cost_estimate=pl.CostEstimate(flops=20000000, bytes_accessed=6000000, transcendentals=0),
        name="pack",
    )(density, tracer, mask, mixed)


def patch_kernel(piece, west, east, packed, out_ref):
    lane = lane_of()
    strips = packed.shape[0]
    blocks = west.shape[0] // BR

    def fill(b, strip, edge, start):
        rim = edge[pl.ds(pl.multiple_of(BR * b, BR), BR), :]
        for v in range(VREGS):
            value = packed[strip, b * VREGS + v]
            for m in range(SLOTS):
                at = piece * m + start
                here = (lane >= at) & (lane < at + HALO)
                value = jnp.where(here, rolled(rim, at - HALO * plane_at(v, m)), value)
            out_ref[strip, b * VREGS + v] = value

    for b in range(blocks):
        fill(b, 0, west, 0)
        fill(b, strips - 1, east, piece - HALO)


def patch(west, east, packed, piece):
    whole = pl.BlockSpec(memory_space=pltpu.VMEM)

    def kernel(*refs):
        patch_kernel(piece, *refs)

    return pl.pallas_call(
        kernel,
        out_shape=jax.ShapeDtypeStruct(packed.shape, jnp.float32),
        in_specs=[whole, whole, whole],
        out_specs=whole,
        input_output_aliases={2: 0},
        compiler_params=pltpu.CompilerParams(vmem_limit_bytes=SMALL),
        name="patch",
    )(west, east, packed)


def sweep_kernel(
    width, blocks, order, owner, got, out_ref, slot_of, rho, ta, tb, cp, cq, cr, sea, mix, kap, me, mw, mn, ms, ce, cw, cn, cs
):
    piece = width + 2 * HALO
    depth = (sea.shape[0] - 2 * BR) // BR
    lane = lane_of()
    first = lane < piece
    second = lane < 2 * piece

    def invert(s, carry):
        slot_of[order[s]] = s
        return carry

    lax.fori_loop(0, blocks, invert, 0, unroll=8)
    for b in range(blocks, SLOTS * depth):
        slot_of[b] = slot_of[0]

    def loop(body, count, chunk):
        def some(i, carry):
            body(i)
            return carry

        lax.fori_loop(0, count // chunk, some, 0)

    def rows(c, off=0, chunk=1):
        start = BR + BR * chunk * c
        if off == 0:
            return pl.ds(pl.multiple_of(start, BR), BR * chunk)
        return pl.ds(start + off, BR * chunk)

    def close(ref):
        top = jnp.where(first, 0.0, rolled(ref[pl.ds(BR * depth, BR), :], piece))
        bottom = jnp.where(second, rolled(ref[pl.ds(BR, BR), :], -piece), 0.0)
        ref[pl.ds(0, BR), :] = top
        ref[pl.ds(BR * (depth + 1), BR), :] = bottom

    def gather(c):
        for u in range(GATHER):
            i = c * GATHER + u
            slots = [slot_of[i + depth * m] for m in range(SLOTS)]
            owners = [owner[s] for s in slots]
            real = jnp.where(i + depth * (SLOTS - 1) < blocks, 1.0, 0.0)

            def plane(v, n, where):
                parts = [rolled(got[where[m], v], piece * (m - n)) for m in range(SLOTS)]
                return jnp.where(first, parts[0], jnp.where(second, parts[1], parts[2] * real))

            at = rows(i)
            for k in range(K):
                rho[k, at, :] = plane(k % 3, k // 3, slots)
                ta[k, at, :] = plane(3 + k % 3, k // 3, owners)
            sea[at, :] = plane(2, 2, slots)
            mix[at, :] = plane(5, 2, slots)

    loop(gather, depth, GATHER)
    for k in range(K):
        close(rho.at[k])
        close(ta.at[k])
    close(sea)

    def physics(c):
        at, up, down = (rows(c, off, PHYSICS) for off in (0, 1, -1))
        mixed = mix[at, :]
        here = sea[at, :]
        east = rolled(here, -1) * here
        west = rolled(here, 1) * here
        north = sea[up, :] * here
        south = sea[down, :] * here
        me[at, :] = east
        mw[at, :] = west
        mn[at, :] = north
        ms[at, :] = south
        per_mixed = 1.0 / (mixed + 1.0)
        f = [rho[k, at, :] for k in range(K)]
        total = jnp.zeros_like(here)
        kept = []
        for k in range(K):
            sum_e = east * (rolled(f[k], -1) - f[k]) + west * (f[k] - rolled(f[k], 1))
            sum_n = north * (rho[k, up, :] - f[k]) + south * (f[k] - rho[k, down, :])
            above, under = max(k - 1, 0), min(k + 1, K - 1)
            rising = 0.5 * STRATIFICATION * (under - above)
            denominator = jnp.maximum(0.5 * (f[under] - f[above]) + rising, DENSITY_FLOOR)
            scale = -0.5 / denominator
            se = sum_e * scale
            sn = sum_n * scale
            squared = se * se + sn * sn
            taper = 0.5 + 0.5 * jnp.tanh((SLOPE_LIMIT - squared) * (1.0 / TAPER_WIDTH))
            factor = taper * jnp.minimum(1.0, (k + 1.0) * per_mixed) * here
            se = se * factor
            sn = sn * factor
            squared = se * se + sn * sn
            root = jnp.sqrt(denominator * (squared + KERNEL_OFFSET))
            total += jnp.where(mixed <= float(k), root, 0.0)
            cp[k, at, :] = se
            cq[k, at, :] = sn
            kept.append(squared)
        kappa = here * (BASE_DIFFUSIVITY + VISBECK_ALPHA * total / (K - mixed))
        kap[at, :] = kappa
        weight = (0.5 * TIME_STEP) * kappa
        for k in range(K):
            cp[k, at, :] = weight * cp[k, at, :]
            cq[k, at, :] = weight * cq[k, at, :]
            cr[k, at, :] = (0.5 * weight) * kept[k]

    loop(physics, depth, PHYSICS)
    close(kap)

    def faces(c):
        at, up, down = (rows(c, off, FACES) for off in (0, 1, -1))
        kappa = (0.5 * TIME_STEP) * kap[at, :]
        ce[at, :] = (kappa + rolled(kappa, -1)) * me[at, :]
        cw[at, :] = (kappa + rolled(kappa, 1)) * mw[at, :]
        cn[at, :] = (kappa + (0.5 * TIME_STEP) * kap[up, :]) * mn[at, :]
        cs[at, :] = (kappa + (0.5 * TIME_STEP) * kap[down, :]) * ms[at, :]

    loop(faces, depth, FACES)

    def advance(c, source, chunk):
        at, up, down = (rows(c, off, chunk) for off in (0, 1, -1))
        mask_e, mask_w, mask_n, mask_s = (ref[at, :] for ref in (me, mw, mn, ms))
        face_e, face_w, face_n, face_s = (ref[at, :] for ref in (ce, cw, cn, cs))
        f = [source[k, at, :] for k in range(K)]
        flux, result = [], []
        for k in range(K):
            step_e = rolled(f[k], -1) - f[k]
            step_w = f[k] - rolled(f[k], 1)
            step_n = source[k, up, :] - f[k]
            step_s = f[k] - source[k, down, :]
            sum_e = mask_e * step_e + mask_w * step_w
            sum_n = mask_n * step_n + mask_s * step_s
            lateral = (face_e * step_e - face_w * step_w) + (face_n * step_n - face_s * step_s)
            drop = f[min(k + 1, K - 1)] - f[max(k - 1, 0)]
            flux.append(cp[k, at, :] * sum_e + cq[k, at, :] * sum_n + cr[k, at, :] * drop)
            result.append(f[k] + lateral)
        for k in range(K):
            if k + 1 < K:
                result[k] += flux[k + 1]
            if k > 0:
                result[k] -= flux[k - 1]
        return result

    def sweep(source, target):
        def body(c):
            result = advance(c, source, SWEEP)
            for k in range(K):
                target[k, rows(c, 0, SWEEP), :] = result[k]

        loop(body, depth, SWEEP)
        for k in range(K):
            close(target.at[k])

    for n in range(ITERS - 1):
        sweep(*((ta, tb) if n % 2 == 0 else (tb, ta)))
    source = ta if (ITERS - 1) % 2 == 0 else tb
    per_out = LANES // width
    wide = lane_of((BR * LAST, LANES))

    def last(back):
        c = depth // LAST - 1 - back
        result = advance(c, source, LAST)
        for g in reversed(range(SLOTS)):
            for h in range(K // per_out):
                value = None
                for m in range(per_out):
                    part = rolled(result[h * per_out + m], width * m - (piece * g + HALO))
                    value = part if m == 0 else jnp.where(wide < width * m, value, part)
                for u in range(LAST):
                    t = owner[slot_of[c * LAST + u + depth * g]]
                    out_ref[t, h] = value[BR * u : BR * (u + 1), :]

    loop(last, depth, LAST)


def sweeps(order, owner, got, width):
    blocks = got.shape[0]
    depth = -(-blocks // (SLOTS * UNIT)) * UNIT
    padded = BR * (depth + 2)
    cube = pltpu.VMEM((K, padded, LANES), jnp.float32)
    flat = pltpu.VMEM((padded, LANES), jnp.float32)
    outs = K * width // LANES

    def kernel(*refs):
        sweep_kernel(width, blocks, *refs)

    return pl.pallas_call(
        kernel,
        out_shape=jax.ShapeDtypeStruct((blocks, outs, BR, LANES), jnp.float32),
        in_specs=[
            pl.BlockSpec(memory_space=pltpu.SMEM),
            pl.BlockSpec(memory_space=pltpu.SMEM),
            pl.BlockSpec(memory_space=pltpu.VMEM),
        ],
        out_specs=pl.BlockSpec(memory_space=pltpu.VMEM),
        scratch_shapes=[pltpu.SMEM((SLOTS * depth,), jnp.int32)] + [cube] * 6 + [flat] * 11,
        compiler_params=pltpu.CompilerParams(vmem_limit_bytes=40 * 1024 * 1024),
        name="sweeps",
    )(order, owner, got)


def unpack_kernel(width, got, out_ref):
    per_tile = LANES // width
    tiles = out_ref.shape[2] // LANES
    count = out_ref.shape[1] // BR
    outs = K // per_tile
    lane = lane_of()
    for u in range(count):
        block = pl.program_id(0) * count + u
        for k in range(K):
            h, m = divmod(k, per_tile)
            for t in range(tiles):
                value = None
                for q in range(per_tile):
                    part = rolled(got[t * per_tile + q, block * outs + h], width * (q - m))
                    value = part if q == 0 else jnp.where(lane < width * q, value, part)
                out_ref[k, BR * u : BR * (u + 1), LANES * t : LANES * (t + 1)] = value


def unpack(got, rows, columns):
    strips = got.shape[0]
    blocks = rows // BR
    width = columns // strips

    def kernel(*refs):
        unpack_kernel(width, *refs)

    return pl.pallas_call(
        kernel,
        grid=(UNPACK,),
        out_shape=jax.ShapeDtypeStruct((K, rows, columns), jnp.float32),
        in_specs=[pl.BlockSpec(memory_space=pltpu.VMEM)],
        out_specs=pl.BlockSpec((K, rows // UNPACK, columns), lambda b: (0, b, 0)),
        compiler_params=pltpu.CompilerParams(vmem_limit_bytes=SMALL),
        name="unpack",
    )(got)


def on_device(density, tracer, sea_mask, mixed_level, tile_blocks, block_owner):
    rows, columns = sea_mask.shape
    strips = lax.axis_size("gy")
    ring = lax.axis_size("gx")
    width = columns // strips
    blocks = rows // BR
    head, tail = edges(density, tracer, sea_mask, mixed_level)
    west = lax.ppermute(tail, "gx", [(i, (i + 1) % ring) for i in range(ring)])
    east = lax.ppermute(head, "gx", [((i + 1) % ring, i) for i in range(ring)])
    packed = pack(density, tracer, sea_mask, mixed_level, strips)
    packed = patch(west, east, packed, width + 2 * HALO)
    got = lax.all_to_all(packed, "gy", split_axis=0, concat_axis=0, tiled=True)
    done = sweeps(tile_blocks, block_owner, got.reshape(strips * blocks, VREGS, BR, LANES), width)
    back = lax.all_to_all(
        done.reshape(strips, -1, BR, LANES), "gy", split_axis=0, concat_axis=0, tiled=True
    )
    return unpack(back, rows, columns)


def solution(mesh):
    placed = (P(None, "gy", "gx"), P(None, "gy", "gx"), P("gy", "gx"), P("gy", "gx"), P(), P())
    return jax.shard_map(
        on_device, mesh=mesh, in_specs=placed, out_specs=P(None, "gy", "gx"), check_vma=False
    )
```

```python
import jax
import jax.numpy as jnp
from jax import lax
from jax.experimental import pallas as pl
from jax.experimental.pallas import tpu as pltpu
from jax.sharding import PartitionSpec as P

K = 8
BR = 8
ITERS = 4
HALO = ITERS + 1
LANES = 128
SLOTS = 3
VREGS = 6
PACK = 2
UNPACK = 2
SMALL = 12 * 1024 * 1024
PLANES = 2 * K + 2
UNIT = 4
DEEPEST = 4
GATHER = 11
PHYSICS = 4
FACES = 22
SWEEP = 4
LAST = 4

TIME_STEP = 0.2
STRATIFICATION = 1.0
DENSITY_FLOOR = 0.25
SLOPE_LIMIT = 1.0
TAPER_WIDTH = 0.5
KERNEL_OFFSET = 0.05
BASE_DIFFUSIVITY = 0.2
VISBECK_ALPHA = 0.5


def rolled(x, shift):
    shift %= LANES
    return x if shift == 0 else pltpu.roll(x, shift, x.ndim - 1)


def lane_of(shape=(BR, LANES)):
    return lax.broadcasted_iota(jnp.int32, shape, len(shape) - 1)


def plane_at(register, piece):
    if piece == 2 and register == 2:
        return 2 * K
    if piece == 2 and register == 5:
        return 2 * K + 1
    return register % 3 + 3 * piece + (K if register >= 3 else 0)


def edges_kernel(first, last, head_ref, tail_ref):
    shape = head_ref.shape
    lane = lane_of(shape)
    for planes, start, out_ref in ((first, 0, head_ref), (last, LANES - HALO, tail_ref)):
        out = jnp.zeros(shape, jnp.float32)
        for p in range(PLANES):
            at = HALO * p
            out = jnp.where((lane >= at) & (lane < at + HALO), rolled(planes[p], at - start), out)
        out_ref[...] = out


def edges(planes):
    rows, columns = planes.shape[1:]
    last = columns // LANES - 1
    rim = pl.BlockSpec((rows, LANES), lambda i: (0, 0))
    out = jax.ShapeDtypeStruct((rows, LANES), jnp.float32)
    return pl.pallas_call(
        edges_kernel,
        grid=(1,),
        out_shape=(out, out),
        in_specs=[
            pl.BlockSpec((PLANES, rows, LANES), lambda i: (0, 0, 0)),
            pl.BlockSpec((PLANES, rows, LANES), lambda i: (0, 0, last)),
        ],
        out_specs=(rim, rim),
        compiler_params=pltpu.CompilerParams(vmem_limit_bytes=SMALL),
        name="edges",
    )(planes, planes)


def pack_kernel(width, planes, out_ref):
    piece = width + 2 * HALO
    per_tile = LANES // width
    tiles = planes.shape[2] // LANES
    count = planes.shape[1] // BR
    lane = lane_of()

    def columns(p, row):
        return [planes[p, row, LANES * t : LANES * (t + 1)] for t in range(tiles)]

    for u in range(count):
        block = pl.program_id(0) * count + u
        for v in range(VREGS):
            whole, seam = [], []
            for m in range(SLOTS):
                own = columns(plane_at(v, m), slice(BR * u, BR * (u + 1)))
                whole.append(own)
                seam.append(
                    [own[0]]
                    + [jnp.where(lane < LANES // 2, own[t], own[t - 1]) for t in range(1, tiles)]
                    + [own[-1]]
                )
            for j in range(tiles * per_tile):
                t, q = divmod(j, per_tile)
                parts = []
                for m in range(SLOTS):
                    if q == 0:
                        source = seam[m][t]
                    elif q == per_tile - 1:
                        source = seam[m][t + 1]
                    else:
                        source = whole[m][t]
                    parts.append(rolled(source, piece * m - (width * q - HALO)))
                out_ref[j, block * VREGS + v] = jnp.where(
                    lane < piece, parts[0], jnp.where(lane < 2 * piece, parts[1], parts[2])
                )


def pack(planes, strips):
    rows, columns = planes.shape[1:]
    blocks = rows // BR
    width = columns // strips

    def kernel(*refs):
        pack_kernel(width, *refs)

    return pl.pallas_call(
        kernel,
        grid=(PACK,),
        out_shape=jax.ShapeDtypeStruct((strips, blocks * VREGS, BR, LANES), jnp.float32),
        in_specs=[pl.BlockSpec((PLANES, rows // PACK, columns), lambda b: (0, b, 0))],
        out_specs=pl.BlockSpec(memory_space=pltpu.VMEM),
        compiler_params=pltpu.CompilerParams(vmem_limit_bytes=SMALL),
        cost_estimate=pl.CostEstimate(flops=20000000, bytes_accessed=6000000, transcendentals=0),
        name="pack",
    )(planes)


def patch_kernel(piece, west, east, packed, out_ref):
    lane = lane_of()
    strips = packed.shape[0]
    blocks = west.shape[0] // BR

    def fill(b, strip, edge, start):
        rim = edge[pl.ds(pl.multiple_of(BR * b, BR), BR), :]
        for v in range(VREGS):
            value = packed[strip, b * VREGS + v]
            for m in range(SLOTS):
                at = piece * m + start
                here = (lane >= at) & (lane < at + HALO)
                value = jnp.where(here, rolled(rim, at - HALO * plane_at(v, m)), value)
            out_ref[strip, b * VREGS + v] = value

    for b in range(blocks):
        fill(b, 0, west, 0)
        fill(b, strips - 1, east, piece - HALO)


def patch(west, east, packed, piece):
    whole = pl.BlockSpec(memory_space=pltpu.VMEM)

    def kernel(*refs):
        patch_kernel(piece, *refs)

    return pl.pallas_call(
        kernel,
        out_shape=jax.ShapeDtypeStruct(packed.shape, jnp.float32),
        in_specs=[whole, whole, whole],
        out_specs=whole,
        input_output_aliases={2: 0},
        compiler_params=pltpu.CompilerParams(vmem_limit_bytes=SMALL),
        name="patch",
    )(west, east, packed)


def sweep_kernel(
    width, blocks, order, owner, got, out_ref, slot_of, rho, ta, tb, cp, cq, cr, sea, mix, kap, me, mw, mn, ms, ce, cw, cn, cs
):
    piece = width + 2 * HALO
    depth = (sea.shape[0] - 2 * BR) // BR
    lane = lane_of()
    first = lane < piece
    second = lane < 2 * piece

    def invert(s, carry):
        slot_of[order[s]] = s
        return carry

    lax.fori_loop(0, blocks, invert, 0, unroll=8)
    for b in range(blocks, SLOTS * depth):
        slot_of[b] = slot_of[0]

    def loop(body, count, chunk):
        def some(i, carry):
            body(i)
            return carry

        lax.fori_loop(0, count // chunk, some, 0)

    def rows(c, off=0, chunk=1):
        start = BR + BR * chunk * c
        if off == 0:
            return pl.ds(pl.multiple_of(start, BR), BR * chunk)
        return pl.ds(start + off, BR * chunk)

    def close(ref):
        top = jnp.where(first, 0.0, rolled(ref[pl.ds(BR * depth, BR), :], piece))
        bottom = jnp.where(second, rolled(ref[pl.ds(BR, BR), :], -piece), 0.0)
        ref[pl.ds(0, BR), :] = top
        ref[pl.ds(BR * (depth + 1), BR), :] = bottom

    def gather(c):
        for u in range(GATHER):
            i = c * GATHER + u
            slots = [slot_of[i + depth * m] for m in range(SLOTS)]
            owners = [owner[s] for s in slots]
            real = jnp.where(i + depth * (SLOTS - 1) < blocks, 1.0, 0.0)

            def plane(v, n, where):
                parts = [rolled(got[where[m], v], piece * (m - n)) for m in range(SLOTS)]
                return jnp.where(first, parts[0], jnp.where(second, parts[1], parts[2] * real))

            at = rows(i)
            for k in range(K):
                rho[k, at, :] = plane(k % 3, k // 3, slots)
                ta[k, at, :] = plane(3 + k % 3, k // 3, owners)
            sea[at, :] = plane(2, 2, slots)
            mix[at, :] = plane(5, 2, slots)

    loop(gather, depth, GATHER)
    for k in range(K):
        close(rho.at[k])
        close(ta.at[k])
    close(sea)

    def physics(c):
        at, up, down = (rows(c, off, PHYSICS) for off in (0, 1, -1))
        mixed = mix[at, :]
        here = sea[at, :]
        east = rolled(here, -1) * here
        west = rolled(here, 1) * here
        north = sea[up, :] * here
        south = sea[down, :] * here
        me[at, :] = east
        mw[at, :] = west
        mn[at, :] = north
        ms[at, :] = south
        per_mixed = 1.0 / (mixed + 1.0)
        f = [rho[k, at, :] for k in range(K)]
        total = jnp.zeros_like(here)
        kept = []
        for k in range(K):
            sum_e = east * (rolled(f[k], -1) - f[k]) + west * (f[k] - rolled(f[k], 1))
            sum_n = north * (rho[k, up, :] - f[k]) + south * (f[k] - rho[k, down, :])
            above, under = max(k - 1, 0), min(k + 1, K - 1)
            rising = STRATIFICATION * (under - above)
            twice = jnp.maximum((f[under] - f[above]) + rising, 2.0 * DENSITY_FLOOR)
            scale = 1.0 / twice
            se = sum_e * scale
            sn = sum_n * scale
            squared = se * se + sn * sn
            taper = 0.5 + 0.5 * jnp.tanh(SLOPE_LIMIT / TAPER_WIDTH - squared * (1.0 / TAPER_WIDTH))
            if k < DEEPEST:
                taper = taper * jnp.minimum(1.0, (k + 1.0) * per_mixed)
            squared = squared * (taper * taper)
            under_root = twice * (squared + KERNEL_OFFSET)
            root = under_root * lax.rsqrt(under_root)
            total += jnp.where(mixed <= float(k), root, 0.0) if k < DEEPEST else root
            cp[k, at, :] = se * taper
            cq[k, at, :] = sn * taper
            kept.append(squared)
        share = (VISBECK_ALPHA * 0.5**0.5) * total / (K - mixed)
        kappa = here * (BASE_DIFFUSIVITY + share)
        kap[at, :] = kappa
        weight = (0.5 * TIME_STEP) * kappa
        for k in range(K):
            cp[k, at, :] = -weight * cp[k, at, :]
            cq[k, at, :] = -weight * cq[k, at, :]
            cr[k, at, :] = (0.5 * weight) * kept[k]

    loop(physics, depth, PHYSICS)
    close(kap)

    def faces(c):
        at, up, down = (rows(c, off, FACES) for off in (0, 1, -1))
        kappa = (0.5 * TIME_STEP) * kap[at, :]
        ce[at, :] = (kappa + rolled(kappa, -1)) * me[at, :]
        cw[at, :] = (kappa + rolled(kappa, 1)) * mw[at, :]
        cn[at, :] = (kappa + (0.5 * TIME_STEP) * kap[up, :]) * mn[at, :]
        cs[at, :] = (kappa + (0.5 * TIME_STEP) * kap[down, :]) * ms[at, :]

    loop(faces, depth, FACES)

    def advance(c, source, chunk):
        at, up, down = (rows(c, off, chunk) for off in (0, 1, -1))
        mask_e, mask_w, mask_n, mask_s = (ref[at, :] for ref in (me, mw, mn, ms))
        face_e, face_w, face_n, face_s = (ref[at, :] for ref in (ce, cw, cn, cs))
        f = [source[k, at, :] for k in range(K)]
        flux, result = [], []
        for k in range(K):
            step_e = rolled(f[k], -1) - f[k]
            step_w = f[k] - rolled(f[k], 1)
            step_n = source[k, up, :] - f[k]
            step_s = f[k] - source[k, down, :]
            sum_e = mask_e * step_e + mask_w * step_w
            sum_n = mask_n * step_n + mask_s * step_s
            lateral = (face_e * step_e - face_w * step_w) + (face_n * step_n - face_s * step_s)
            drop = f[min(k + 1, K - 1)] - f[max(k - 1, 0)]
            flux.append(cp[k, at, :] * sum_e + cq[k, at, :] * sum_n + cr[k, at, :] * drop)
            result.append(f[k] + lateral)
        for k in range(K):
            if k + 1 < K:
                result[k] += flux[k + 1]
            if k > 0:
                result[k] -= flux[k - 1]
        return result

    def sweep(source, target):
        def body(c):
            result = advance(c, source, SWEEP)
            for k in range(K):
                target[k, rows(c, 0, SWEEP), :] = result[k]

        loop(body, depth, SWEEP)
        for k in range(K):
            close(target.at[k])

    for n in range(ITERS - 1):
        sweep(*((ta, tb) if n % 2 == 0 else (tb, ta)))
    source = ta if (ITERS - 1) % 2 == 0 else tb
    per_out = LANES // width
    wide = lane_of((BR * LAST, LANES))

    target = tb if source is ta else ta
    chunks = depth // LAST

    def repack(c):
        result = [target[k, rows(c, 0, LAST), :] for k in range(K)]
        for g in reversed(range(SLOTS)):
            for h in range(K // per_out):
                value = None
                for m in range(per_out):
                    part = rolled(result[h * per_out + m], width * m - (piece * g + HALO))
                    value = part if m == 0 else jnp.where(wide < width * m, value, part)
                for u in range(LAST):
                    t = owner[slot_of[c * LAST + u + depth * g]]
                    out_ref[t, h] = value[BR * u : BR * (u + 1), :]

    def final(c):
        result = advance(c, source, LAST)
        for k in range(K):
            target[k, rows(c, 0, LAST), :] = result[k]

    def last(back, carry):
        repack(chunks - back)
        final(chunks - 1 - back)
        return carry

    final(chunks - 1)
    lax.fori_loop(1, chunks, last, 0)
    repack(0)


def sweeps(order, owner, got, width):
    blocks = got.shape[0]
    depth = -(-blocks // (SLOTS * UNIT)) * UNIT
    padded = BR * (depth + 2)
    cube = pltpu.VMEM((K, padded, LANES), jnp.float32)
    flat = pltpu.VMEM((padded, LANES), jnp.float32)
    outs = K * width // LANES

    def kernel(*refs):
        sweep_kernel(width, blocks, *refs)

    return pl.pallas_call(
        kernel,
        out_shape=jax.ShapeDtypeStruct((blocks, outs, BR, LANES), jnp.float32),
        in_specs=[
            pl.BlockSpec(memory_space=pltpu.SMEM),
            pl.BlockSpec(memory_space=pltpu.SMEM),
            pl.BlockSpec(memory_space=pltpu.VMEM),
        ],
        out_specs=pl.BlockSpec(memory_space=pltpu.VMEM),
        scratch_shapes=[pltpu.SMEM((SLOTS * depth,), jnp.int32)] + [cube] * 6 + [flat] * 11,
        compiler_params=pltpu.CompilerParams(vmem_limit_bytes=40 * 1024 * 1024),
        name="sweeps",
    )(order, owner, got)


def unpack_kernel(width, got, out_ref):
    per_tile = LANES // width
    tiles = out_ref.shape[2] // LANES
    count = out_ref.shape[1] // BR
    outs = K // per_tile
    lane = lane_of()
    for u in range(count):
        block = pl.program_id(0) * count + u
        for k in range(K):
            h, m = divmod(k, per_tile)
            for t in range(tiles):
                value = None
                for q in range(per_tile):
                    part = rolled(got[t * per_tile + q, block * outs + h], width * (q - m))
                    value = part if q == 0 else jnp.where(lane < width * q, value, part)
                out_ref[k, BR * u : BR * (u + 1), LANES * t : LANES * (t + 1)] = value


def unpack(got, rows, columns):
    strips = got.shape[0]
    blocks = rows // BR
    width = columns // strips

    def kernel(*refs):
        unpack_kernel(width, *refs)

    return pl.pallas_call(
        kernel,
        grid=(UNPACK,),
        out_shape=jax.ShapeDtypeStruct((K, rows, columns), jnp.float32),
        in_specs=[pl.BlockSpec(memory_space=pltpu.VMEM)],
        out_specs=pl.BlockSpec((K, rows // UNPACK, columns), lambda b: (0, b, 0)),
        compiler_params=pltpu.CompilerParams(vmem_limit_bytes=SMALL),
        name="unpack",
    )(got)


def on_device(density, tracer, sea_mask, mixed_level, tile_blocks, block_owner):
    rows, columns = sea_mask.shape
    strips = lax.axis_size("gy")
    ring = lax.axis_size("gx")
    width = columns // strips
    blocks = rows // BR
    flats = [flat[None].astype(jnp.float32) for flat in (sea_mask, mixed_level)]
    planes = jnp.concatenate([density, tracer, *flats])
    head, tail = edges(planes)
    west = lax.ppermute(tail, "gx", [(i, (i + 1) % ring) for i in range(ring)])
    east = lax.ppermute(head, "gx", [((i + 1) % ring, i) for i in range(ring)])
    packed = pack(planes, strips)
    packed = patch(west, east, packed, width + 2 * HALO)
    got = lax.all_to_all(packed, "gy", split_axis=0, concat_axis=0, tiled=True)
    done = sweeps(tile_blocks, block_owner, got.reshape(strips * blocks, VREGS, BR, LANES), width)
    back = lax.all_to_all(
        done.reshape(strips, -1, BR, LANES), "gy", split_axis=0, concat_axis=0, tiled=True
    )
    return unpack(back, rows, columns)


def solution(mesh):
    placed = (P(None, "gy", "gx"), P(None, "gy", "gx"), P("gy", "gx"), P("gy", "gx"), P(), P())
    return jax.shard_map(
        on_device, mesh=mesh, in_specs=placed, out_specs=P(None, "gy", "gx"), check_vma=False
    )
```

```python
import jax
import jax.numpy as jnp
from jax import lax
from jax.experimental import pallas as pl
from jax.experimental.pallas import tpu as pltpu
from jax.sharding import PartitionSpec as P

K = 8
BR = 8
ITERS = 4
HALO = ITERS + 1
LANES = 128
SLOTS = 3
VREGS = 6
UNPACK = 2
SMALL = 12 * 1024 * 1024
PLANES = 2 * K + 2
UNIT = 4
DEEPEST = 4
GATHER = 4
PHYSICS = 4
FACES = 22
SWEEP = 4
LAST = 4

TIME_STEP = 0.2
STRATIFICATION = 1.0
DENSITY_FLOOR = 0.25
SLOPE_LIMIT = 1.0
TAPER_WIDTH = 0.5
KERNEL_OFFSET = 0.05
BASE_DIFFUSIVITY = 0.2
VISBECK_ALPHA = 0.5


def rolled(x, shift):
    shift %= LANES
    return x if shift == 0 else pltpu.roll(x, shift, x.ndim - 1)


def lane_of(shape=(BR, LANES)):
    return lax.broadcasted_iota(jnp.int32, shape, len(shape) - 1)


def plane_at(register, piece):
    if piece == 2 and register == 2:
        return 2 * K
    if piece == 2 and register == 5:
        return 2 * K + 1
    return register % 3 + 3 * piece + (K if register >= 3 else 0)


def edges_kernel(planes, head_ref, tail_ref):
    shape = head_ref.shape
    lane = lane_of(shape)
    last = planes.shape[2] - LANES
    for start, edge, out_ref in ((0, 0, head_ref), (last, LANES - HALO, tail_ref)):
        out = jnp.zeros(shape, jnp.float32)
        for p in range(PLANES):
            at = HALO * p
            plane = rolled(planes[p, :, start : start + LANES], at - edge)
            out = jnp.where((lane >= at) & (lane < at + HALO), plane, out)
        out_ref[...] = out


def edges(planes):
    whole = pl.BlockSpec(memory_space=pltpu.VMEM)
    out = jax.ShapeDtypeStruct((planes.shape[1], LANES), jnp.float32)
    return pl.pallas_call(
        edges_kernel,
        out_shape=(out, out),
        in_specs=[whole],
        out_specs=(whole, whole),
        compiler_params=pltpu.CompilerParams(vmem_limit_bytes=SMALL),
        name="edges",
    )(planes)


def pack_kernel(width, planes, out_ref):
    piece = width + 2 * HALO
    per_tile = LANES // width
    tiles = planes.shape[2] // LANES
    lane = lane_of()

    def below(limit, start):
        return ((lane - start) & (LANES - 1)) < limit

    west_half = [below(LANES // 2, piece * m) for m in range(SLOTS)]
    one = [below(piece, width * q - HALO) for q in range(per_tile)]
    two = [below(2 * piece, width * q - HALO) for q in range(per_tile)]

    for b in range(planes.shape[1] // BR):
        for v in range(VREGS):
            whole, seam = [], []
            for m in range(SLOTS):
                own = [
                    rolled(
                        planes[plane_at(v, m), BR * b : BR * (b + 1), LANES * t : LANES * (t + 1)],
                        piece * m,
                    )
                    for t in range(tiles)
                ]
                whole.append(own)
                seam.append(
                    [own[0]]
                    + [jnp.where(west_half[m], own[t], own[t - 1]) for t in range(1, tiles)]
                    + [own[-1]]
                )
            for j in range(tiles * per_tile):
                t, q = divmod(j, per_tile)
                if q == 0:
                    parts = [seam[m][t] for m in range(SLOTS)]
                elif q == per_tile - 1:
                    parts = [seam[m][t + 1] for m in range(SLOTS)]
                else:
                    parts = [whole[m][t] for m in range(SLOTS)]
                out_ref[j, b * VREGS + v] = jnp.where(one[q], parts[0], jnp.where(two[q], parts[1], parts[2]))


def pack(planes, strips):
    rows, columns = planes.shape[1:]
    whole = pl.BlockSpec(memory_space=pltpu.VMEM)
    width = columns // strips

    def kernel(*refs):
        pack_kernel(width, *refs)

    return pl.pallas_call(
        kernel,
        out_shape=jax.ShapeDtypeStruct((strips, rows // BR * VREGS, BR, LANES), jnp.float32),
        in_specs=[whole],
        out_specs=whole,
        compiler_params=pltpu.CompilerParams(vmem_limit_bytes=SMALL),
        cost_estimate=pl.CostEstimate(flops=20000000, bytes_accessed=6000000, transcendentals=0),
        name="pack",
    )(planes)


def patch_kernel(width, west, east, packed, out_ref):
    piece = width + 2 * HALO
    lane = lane_of()
    strips = packed.shape[0]

    def fill(b, strip, edge, start):
        rim = edge[BR * b : BR * (b + 1), :]
        for v in range(VREGS):
            value = packed[strip, b * VREGS + v]
            for m in range(SLOTS):
                at = (piece * m + start) % LANES
                here = (lane >= at) & (lane < at + HALO)
                value = jnp.where(here, rolled(rim, at - HALO * plane_at(v, m)), value)
            out_ref[strip, b * VREGS + v] = value

    for b in range(west.shape[0] // BR):
        fill(b, 0, west, LANES - HALO)
        fill(b, strips - 1, east, 0)


def patch(west, east, packed, width):
    whole = pl.BlockSpec(memory_space=pltpu.VMEM)

    def kernel(*refs):
        patch_kernel(width, *refs)

    return pl.pallas_call(
        kernel,
        out_shape=jax.ShapeDtypeStruct(packed.shape, jnp.float32),
        in_specs=[whole, whole, whole],
        out_specs=whole,
        input_output_aliases={2: 0},
        compiler_params=pltpu.CompilerParams(vmem_limit_bytes=SMALL),
        name="patch",
    )(west, east, packed)


def sweep_kernel(
    width, blocks, order, owner, got, out_ref, slot_of, rho, ta, tb, cp, cq, cr, sea, mix, kap, me, mw, mn, ms, ce, cw, cn, cs
):
    piece = width + 2 * HALO
    depth = (sea.shape[0] - 2 * BR) // BR
    strip = lax.axis_index("gy") % (LANES // width)

    def lane_from(start, shape=(BR, LANES)):
        return (lane_of(shape) - (width * strip + (start - HALO))) & (LANES - 1)

    lane = lane_from(0)
    first = lane < piece
    second = lane < 2 * piece

    def invert(s, carry):
        slot_of[order[s]] = s
        return carry

    lax.fori_loop(0, blocks, invert, 0, unroll=8)
    for b in range(blocks, SLOTS * depth):
        slot_of[b] = slot_of[0]

    def loop(body, count, chunk):
        def some(i, carry):
            body(i)
            return carry

        lax.fori_loop(0, count // chunk, some, 0)

    def rows(c, off=0, chunk=1):
        start = BR + BR * chunk * c
        if off == 0:
            return pl.ds(pl.multiple_of(start, BR), BR * chunk)
        return pl.ds(start + off, BR * chunk)

    def close(ref):
        top = jnp.where(first, 0.0, rolled(ref[pl.ds(BR * depth, BR), :], piece))
        bottom = jnp.where(second, rolled(ref[pl.ds(BR, BR), :], -piece), 0.0)
        ref[pl.ds(0, BR), :] = top
        ref[pl.ds(BR * (depth + 1), BR), :] = bottom

    one = [lane_from(piece * n) < piece for n in range(SLOTS)]
    two = [lane_from(piece * n) < 2 * piece for n in range(SLOTS)]

    def gather(c):
        for u in range(GATHER):
            i = c * GATHER + u
            slots = [slot_of[i + depth * m] for m in range(SLOTS)]
            owners = [owner[s] for s in slots]
            real = jnp.where(i + depth * (SLOTS - 1) < blocks, 1.0, 0.0)
            at = rows(i)
            for v in range(VREGS):
                where = slots if v < 3 else owners
                parts = [got[where[m], v] for m in range(SLOTS)]
                parts[2] = parts[2] * real
                parts = [rolled(parts[m], piece * m) for m in range(SLOTS)]
                for n in range(SLOTS):
                    plane = jnp.where(one[n], parts[0], jnp.where(two[n], parts[1], parts[2]))
                    plane = rolled(plane, -piece * n)
                    p = plane_at(v, n)
                    if p < K:
                        rho[p, at, :] = plane
                    elif p < 2 * K:
                        ta[p - K, at, :] = plane
                    elif p == 2 * K:
                        sea[at, :] = plane
            levels = [got[slots[m], 5] for m in range(SLOTS)]
            levels[2] = levels[2] * real
            levels = [rolled(levels[m], piece * m) for m in range(SLOTS)]
            mix[at, :] = rolled(jnp.where(one[2], levels[0], jnp.where(two[2], levels[1], levels[2])), -2 * piece)

    loop(gather, depth, GATHER)
    for k in range(K):
        close(rho.at[k])
        close(ta.at[k])
    close(sea)

    def physics(c):
        at, up, down = (rows(c, off, PHYSICS) for off in (0, 1, -1))
        mixed = mix[at, :]
        here = sea[at, :]
        east = rolled(here, -1) * here
        west = rolled(here, 1) * here
        north = sea[up, :] * here
        south = sea[down, :] * here
        me[at, :] = east
        mw[at, :] = west
        mn[at, :] = north
        ms[at, :] = south
        per_mixed = 1.0 / (mixed + 1.0)
        f = [rho[k, at, :] for k in range(K)]
        total = jnp.zeros_like(here)
        kept = []
        for k in range(K):
            sum_e = east * (rolled(f[k], -1) - f[k]) + west * (f[k] - rolled(f[k], 1))
            sum_n = north * (rho[k, up, :] - f[k]) + south * (f[k] - rho[k, down, :])
            above, under = max(k - 1, 0), min(k + 1, K - 1)
            rising = STRATIFICATION * (under - above)
            twice = jnp.maximum((f[under] - f[above]) + rising, 2.0 * DENSITY_FLOOR)
            scale = 1.0 / twice
            se = sum_e * scale
            sn = sum_n * scale
            squared = se * se + sn * sn
            taper = 0.5 + 0.5 * jnp.tanh(SLOPE_LIMIT / TAPER_WIDTH - squared * (1.0 / TAPER_WIDTH))
            if k < DEEPEST:
                taper = taper * jnp.minimum(1.0, (k + 1.0) * per_mixed)
            squared = squared * (taper * taper)
            under_root = twice * (squared + KERNEL_OFFSET)
            root = under_root * lax.rsqrt(under_root)
            total += jnp.where(mixed <= float(k), root, 0.0) if k < DEEPEST else root
            cp[k, at, :] = se * taper
            cq[k, at, :] = sn * taper
            kept.append(squared)
        share = (VISBECK_ALPHA * 0.5**0.5) * total / (K - mixed)
        kappa = here * (BASE_DIFFUSIVITY + share)
        kap[at, :] = kappa
        weight = (0.5 * TIME_STEP) * kappa
        for k in range(K):
            cp[k, at, :] = -weight * cp[k, at, :]
            cq[k, at, :] = -weight * cq[k, at, :]
            cr[k, at, :] = (0.5 * weight) * kept[k]

    loop(physics, depth, PHYSICS)
    close(kap)

    def faces(c):
        at, up, down = (rows(c, off, FACES) for off in (0, 1, -1))
        kappa = (0.5 * TIME_STEP) * kap[at, :]
        ce[at, :] = (kappa + rolled(kappa, -1)) * me[at, :]
        cw[at, :] = (kappa + rolled(kappa, 1)) * mw[at, :]
        cn[at, :] = (kappa + (0.5 * TIME_STEP) * kap[up, :]) * mn[at, :]
        cs[at, :] = (kappa + (0.5 * TIME_STEP) * kap[down, :]) * ms[at, :]

    loop(faces, depth, FACES)

    def advance(c, source, chunk):
        at, up, down = (rows(c, off, chunk) for off in (0, 1, -1))
        mask_e, mask_w, mask_n, mask_s = (ref[at, :] for ref in (me, mw, mn, ms))
        face_e, face_w, face_n, face_s = (ref[at, :] for ref in (ce, cw, cn, cs))
        f = [source[k, at, :] for k in range(K)]
        flux, result = [], []
        for k in range(K):
            step_e = rolled(f[k], -1) - f[k]
            step_w = f[k] - rolled(f[k], 1)
            step_n = source[k, up, :] - f[k]
            step_s = f[k] - source[k, down, :]
            sum_e = mask_e * step_e + mask_w * step_w
            sum_n = mask_n * step_n + mask_s * step_s
            lateral = (face_e * step_e - face_w * step_w) + (face_n * step_n - face_s * step_s)
            drop = f[min(k + 1, K - 1)] - f[max(k - 1, 0)]
            flux.append(cp[k, at, :] * sum_e + cq[k, at, :] * sum_n + cr[k, at, :] * drop)
            result.append(f[k] + lateral)
        for k in range(K):
            if k + 1 < K:
                result[k] += flux[k + 1]
            if k > 0:
                result[k] -= flux[k - 1]
        return result

    def sweep(source, target):
        def body(c):
            result = advance(c, source, SWEEP)
            for k in range(K):
                target[k, rows(c, 0, SWEEP), :] = result[k]

        loop(body, depth, SWEEP)
        for k in range(K):
            close(target.at[k])

    for n in range(ITERS - 1):
        sweep(*((ta, tb) if n % 2 == 0 else (tb, ta)))
    source = ta if (ITERS - 1) % 2 == 0 else tb
    per_out = LANES // width

    target = tb if source is ta else ta
    chunks = depth // LAST

    inner = [lane_from(piece * g + HALO, (BR * LAST, LANES)) for g in range(SLOTS)]

    def repack(c):
        for h in range(K // per_out):
            levels = [
                rolled(target[h * per_out + m, rows(c, 0, LAST), :], width * m) for m in range(per_out)
            ]
            for g in reversed(range(SLOTS)):
                value = levels[-1]
                for m in reversed(range(per_out - 1)):
                    value = jnp.where(inner[g] < width * (m + 1), levels[m], value)
                value = rolled(value, -piece * g)
                for u in range(LAST):
                    t = owner[slot_of[c * LAST + u + depth * g]]
                    out_ref[t, h] = value[BR * u : BR * (u + 1), :]

    def final(c):
        result = advance(c, source, LAST)
        for k in range(K):
            target[k, rows(c, 0, LAST), :] = result[k]

    def last(back, carry):
        repack(chunks - back)
        final(chunks - 1 - back)
        return carry

    final(chunks - 1)
    lax.fori_loop(1, chunks, last, 0)
    repack(0)


def sweeps(order, owner, got, width):
    blocks = got.shape[0]
    depth = -(-blocks // (SLOTS * UNIT)) * UNIT
    padded = BR * (depth + 2)
    cube = pltpu.VMEM((K, padded, LANES), jnp.float32)
    flat = pltpu.VMEM((padded, LANES), jnp.float32)
    outs = K * width // LANES

    def kernel(*refs):
        sweep_kernel(width, blocks, *refs)

    return pl.pallas_call(
        kernel,
        out_shape=jax.ShapeDtypeStruct((blocks, outs, BR, LANES), jnp.float32),
        in_specs=[
            pl.BlockSpec(memory_space=pltpu.SMEM),
            pl.BlockSpec(memory_space=pltpu.SMEM),
            pl.BlockSpec(memory_space=pltpu.VMEM),
        ],
        out_specs=pl.BlockSpec(memory_space=pltpu.VMEM),
        scratch_shapes=[pltpu.SMEM((SLOTS * depth,), jnp.int32)] + [cube] * 6 + [flat] * 11,
        compiler_params=pltpu.CompilerParams(vmem_limit_bytes=40 * 1024 * 1024),
        name="sweeps",
    )(order, owner, got)


def unpack_kernel(width, got, out_ref):
    per_tile = LANES // width
    tiles = out_ref.shape[2] // LANES
    count = out_ref.shape[1] // BR
    outs = K // per_tile
    place = lane_of() // width
    for u in range(count):
        block = pl.program_id(0) * count + u
        for h in range(outs):
            for t in range(tiles):
                strips = [got[t * per_tile + q, block * outs + h] for q in range(per_tile)]
                for m in range(per_tile):
                    value = strips[-1]
                    for q in range(per_tile - 1):
                        value = jnp.where(place == (m + q) % per_tile, strips[q], value)
                    out_ref[
                        h * per_tile + m, BR * u : BR * (u + 1), LANES * t : LANES * (t + 1)
                    ] = rolled(value, -width * m)


def unpack(got, rows, columns):
    strips = got.shape[0]
    blocks = rows // BR
    width = columns // strips

    def kernel(*refs):
        unpack_kernel(width, *refs)

    return pl.pallas_call(
        kernel,
        grid=(UNPACK,),
        out_shape=jax.ShapeDtypeStruct((K, rows, columns), jnp.float32),
        in_specs=[pl.BlockSpec(memory_space=pltpu.VMEM)],
        out_specs=pl.BlockSpec((K, rows // UNPACK, columns), lambda b: (0, b, 0)),
        compiler_params=pltpu.CompilerParams(vmem_limit_bytes=SMALL),
        name="unpack",
    )(got)


def on_device(density, tracer, sea_mask, mixed_level, tile_blocks, block_owner):
    rows, columns = sea_mask.shape
    strips = lax.axis_size("gy")
    ring = lax.axis_size("gx")
    width = columns // strips
    blocks = rows // BR
    flats = [flat[None].astype(jnp.float32) for flat in (sea_mask, mixed_level)]
    planes = jnp.concatenate([density, tracer, *flats])
    head, tail = edges(planes)
    west = lax.ppermute(tail, "gx", [(i, (i + 1) % ring) for i in range(ring)])
    east = lax.ppermute(head, "gx", [((i + 1) % ring, i) for i in range(ring)])
    packed = pack(planes, strips)
    packed = patch(west, east, packed, width)
    got = lax.all_to_all(packed, "gy", split_axis=0, concat_axis=0, tiled=True)
    done = sweeps(tile_blocks, block_owner, got.reshape(strips * blocks, VREGS, BR, LANES), width)
    back = lax.all_to_all(
        done.reshape(strips, -1, BR, LANES), "gy", split_axis=0, concat_axis=0, tiled=True
    )
    return unpack(back, rows, columns)


def solution(mesh):
    placed = (P(None, "gy", "gx"), P(None, "gy", "gx"), P("gy", "gx"), P("gy", "gx"), P(), P())
    return jax.shard_map(
        on_device, mesh=mesh, in_specs=placed, out_specs=P(None, "gy", "gx"), check_vma=False
    )
```

```python
import jax
import jax.numpy as jnp
from jax import lax
from jax.experimental import pallas as pl
from jax.experimental.pallas import tpu as pltpu
from jax.sharding import PartitionSpec as P

K = 8
BR = 8
ITERS = 4
HALO = ITERS + 1
LANES = 128
SLOTS = 3
VREGS = 6
UNPACK = 2
SMALL = 12 * 1024 * 1024
PLANES = 2 * K + 2
UNIT = 4
DEEPEST = 4
GATHER = 4
PHYSICS = 4
FACES = 22
SWEEP = 4
LAST = 4

TIME_STEP = 0.2
STRATIFICATION = 1.0
DENSITY_FLOOR = 0.25
SLOPE_LIMIT = 1.0
TAPER_WIDTH = 0.5
KERNEL_OFFSET = 0.05
BASE_DIFFUSIVITY = 0.2
VISBECK_ALPHA = 0.5


def rolled(x, shift):
    shift %= LANES
    return x if shift == 0 else pltpu.roll(x, shift, x.ndim - 1)


def lane_of(shape=(BR, LANES)):
    return lax.broadcasted_iota(jnp.int32, shape, len(shape) - 1)


def plane_at(register, piece):
    if piece == 2 and register == 2:
        return 2 * K
    if piece == 2 and register == 5:
        return 2 * K + 1
    return register % 3 + 3 * piece + (K if register >= 3 else 0)


def plane_of(planes, mask, mixed, p, rows, columns):
    if p < 2 * K:
        return planes[p, rows, columns]
    return (mask if p == 2 * K else mixed)[rows, columns].astype(jnp.float32)


def edges_kernel(planes, mask, mixed, near_ref, far_ref):
    shape = near_ref.shape
    lane = lane_of(shape)
    last = planes.shape[2] - LANES
    sides = []
    for start, edge in ((0, 0), (last, LANES - HALO)):
        out = jnp.zeros(shape, jnp.float32)
        for p in range(PLANES):
            at = HALO * p
            plane = plane_of(planes, mask, mixed, p, slice(None), slice(start, start + LANES))
            plane = rolled(plane, at - edge)
            out = jnp.where((lane >= at) & (lane < at + HALO), plane, out)
        sides.append(out)
    head, tail = sides
    even = lax.axis_index("gx") % 2 == 0
    near_ref[...] = jnp.where(even, tail, head)
    far_ref[...] = jnp.where(even, head, tail)


def edges(planes, mask, mixed):
    whole = pl.BlockSpec(memory_space=pltpu.VMEM)
    out = jax.ShapeDtypeStruct((planes.shape[1], LANES), jnp.float32)
    return pl.pallas_call(
        edges_kernel,
        out_shape=(out, out),
        in_specs=[whole, whole, whole],
        out_specs=(whole, whole),
        compiler_params=pltpu.CompilerParams(vmem_limit_bytes=SMALL),
        name="edges",
    )(planes, mask, mixed)


def pack_kernel(width, planes, mask, mixed, out_ref):
    piece = width + 2 * HALO
    per_tile = LANES // width
    tiles = planes.shape[2] // LANES
    lane = lane_of()

    def below(limit, start):
        return ((lane - start) & (LANES - 1)) < limit

    west_half = [below(LANES // 2, piece * m) for m in range(SLOTS)]
    one = [below(piece, width * q - HALO) for q in range(per_tile)]
    two = [below(2 * piece, width * q - HALO) for q in range(per_tile)]

    for b in range(planes.shape[1] // BR):
        for v in range(VREGS):
            whole, seam = [], []
            for m in range(SLOTS):
                own = [
                    rolled(
                        plane_of(
                            planes,
                            mask,
                            mixed,
                            plane_at(v, m),
                            slice(BR * b, BR * (b + 1)),
                            slice(LANES * t, LANES * (t + 1)),
                        ),
                        piece * m,
                    )
                    for t in range(tiles)
                ]
                whole.append(own)
                seam.append(
                    [own[0]]
                    + [jnp.where(west_half[m], own[t], own[t - 1]) for t in range(1, tiles)]
                    + [own[-1]]
                )
            for j in range(tiles * per_tile):
                t, q = divmod(j, per_tile)
                if q == 0:
                    parts = [seam[m][t] for m in range(SLOTS)]
                elif q == per_tile - 1:
                    parts = [seam[m][t + 1] for m in range(SLOTS)]
                else:
                    parts = [whole[m][t] for m in range(SLOTS)]
                out_ref[j, b * VREGS + v] = jnp.where(one[q], parts[0], jnp.where(two[q], parts[1], parts[2]))


def pack(planes, mask, mixed, strips):
    rows, columns = planes.shape[1:]
    whole = pl.BlockSpec(memory_space=pltpu.VMEM)
    width = columns // strips

    def kernel(*refs):
        pack_kernel(width, *refs)

    return pl.pallas_call(
        kernel,
        out_shape=jax.ShapeDtypeStruct((strips, rows // BR * VREGS, BR, LANES), jnp.float32),
        in_specs=[whole, whole, whole],
        out_specs=whole,
        compiler_params=pltpu.CompilerParams(vmem_limit_bytes=SMALL),
        cost_estimate=pl.CostEstimate(flops=20000000, bytes_accessed=6000000, transcendentals=0),
        name="pack",
    )(planes, mask, mixed)


def patch_kernel(width, near, far, packed, out_ref):
    piece = width + 2 * HALO
    even = lax.axis_index("gx") % 2 == 0
    lane = lane_of()
    strips = packed.shape[0]

    def fill(b, strip, evens, odds, start):
        here = slice(BR * b, BR * (b + 1))
        rim = jnp.where(even, evens[here, :], odds[here, :])
        for v in range(VREGS):
            value = packed[strip, b * VREGS + v]
            for m in range(SLOTS):
                at = (piece * m + start) % LANES
                here = (lane >= at) & (lane < at + HALO)
                value = jnp.where(here, rolled(rim, at - HALO * plane_at(v, m)), value)
            out_ref[strip, b * VREGS + v] = value

    for b in range(near.shape[0] // BR):
        fill(b, 0, far, near, LANES - HALO)
        fill(b, strips - 1, near, far, 0)


def patch(near, far, packed, width):
    whole = pl.BlockSpec(memory_space=pltpu.VMEM)

    def kernel(*refs):
        patch_kernel(width, *refs)

    return pl.pallas_call(
        kernel,
        out_shape=jax.ShapeDtypeStruct(packed.shape, jnp.float32),
        in_specs=[whole, whole, whole],
        out_specs=whole,
        input_output_aliases={2: 0},
        compiler_params=pltpu.CompilerParams(vmem_limit_bytes=SMALL),
        name="patch",
    )(near, far, packed)


def sweep_kernel(
    width, blocks, order, owner, got, out_ref, slot_of, rho, ta, tb, cp, cq, cr, sea, mix, kap, me, mw, mn, ms, ce, cw, cn, cs
):
    piece = width + 2 * HALO
    depth = (sea.shape[0] - 2 * BR) // BR
    strip = lax.axis_index("gy") % (LANES // width)

    def lane_from(start, shape=(BR, LANES)):
        return (lane_of(shape) - (width * strip + (start - HALO))) & (LANES - 1)

    lane = lane_from(0)
    first = lane < piece
    second = lane < 2 * piece

    def invert(s, carry):
        slot_of[order[s]] = s
        return carry

    lax.fori_loop(0, blocks, invert, 0, unroll=8)
    for b in range(blocks, SLOTS * depth):
        slot_of[b] = slot_of[0]

    def loop(body, count, chunk):
        def some(i, carry):
            body(i)
            return carry

        lax.fori_loop(0, count // chunk, some, 0)

    def rows(c, off=0, chunk=1):
        start = BR + BR * chunk * c
        if off == 0:
            return pl.ds(pl.multiple_of(start, BR), BR * chunk)
        return pl.ds(start + off, BR * chunk)

    def close(ref):
        top = jnp.where(first, 0.0, rolled(ref[pl.ds(BR * depth, BR), :], piece))
        bottom = jnp.where(second, rolled(ref[pl.ds(BR, BR), :], -piece), 0.0)
        ref[pl.ds(0, BR), :] = top
        ref[pl.ds(BR * (depth + 1), BR), :] = bottom

    one = [lane_from(piece * n) < piece for n in range(SLOTS)]
    two = [lane_from(piece * n) < 2 * piece for n in range(SLOTS)]

    def gather(c):
        for u in range(GATHER):
            i = c * GATHER + u
            slots = [slot_of[i + depth * m] for m in range(SLOTS)]
            owners = [owner[s] for s in slots]
            real = jnp.where(i + depth * (SLOTS - 1) < blocks, 1.0, 0.0)
            at = rows(i)
            for v in range(VREGS):
                where = slots if v < 3 else owners
                parts = [got[where[m], v] for m in range(SLOTS)]
                parts[2] = parts[2] * real
                parts = [rolled(parts[m], piece * m) for m in range(SLOTS)]
                for n in range(SLOTS):
                    plane = jnp.where(one[n], parts[0], jnp.where(two[n], parts[1], parts[2]))
                    plane = rolled(plane, -piece * n)
                    p = plane_at(v, n)
                    if p < K:
                        rho[p, at, :] = plane
                    elif p < 2 * K:
                        ta[p - K, at, :] = plane
                    elif p == 2 * K:
                        sea[at, :] = plane
            levels = [got[slots[m], 5] for m in range(SLOTS)]
            levels[2] = levels[2] * real
            levels = [rolled(levels[m], piece * m) for m in range(SLOTS)]
            mix[at, :] = rolled(jnp.where(one[2], levels[0], jnp.where(two[2], levels[1], levels[2])), -2 * piece)

    loop(gather, depth, GATHER)
    for k in range(K):
        close(rho.at[k])
        close(ta.at[k])
    close(sea)

    def physics(c):
        at, up, down = (rows(c, off, PHYSICS) for off in (0, 1, -1))
        mixed = mix[at, :]
        here = sea[at, :]
        east = rolled(here, -1) * here
        west = rolled(here, 1) * here
        north = sea[up, :] * here
        south = sea[down, :] * here
        me[at, :] = east
        mw[at, :] = west
        mn[at, :] = north
        ms[at, :] = south
        per_mixed = 1.0 / (mixed + 1.0)
        f = [rho[k, at, :] for k in range(K)]
        total = jnp.zeros_like(here)
        kept = []
        for k in range(K):
            sum_e = east * (rolled(f[k], -1) - f[k]) + west * (f[k] - rolled(f[k], 1))
            sum_n = north * (rho[k, up, :] - f[k]) + south * (f[k] - rho[k, down, :])
            above, under = max(k - 1, 0), min(k + 1, K - 1)
            rising = STRATIFICATION * (under - above)
            twice = jnp.maximum((f[under] - f[above]) + rising, 2.0 * DENSITY_FLOOR)
            scale = 1.0 / twice
            se = sum_e * scale
            sn = sum_n * scale
            squared = se * se + sn * sn
            taper = 0.5 + 0.5 * jnp.tanh(SLOPE_LIMIT / TAPER_WIDTH - squared * (1.0 / TAPER_WIDTH))
            if k < DEEPEST:
                taper = taper * jnp.minimum(1.0, (k + 1.0) * per_mixed)
            squared = squared * (taper * taper)
            under_root = twice * (squared + KERNEL_OFFSET)
            root = under_root * lax.rsqrt(under_root)
            total += jnp.where(mixed <= float(k), root, 0.0) if k < DEEPEST else root
            cp[k, at, :] = se * taper
            cq[k, at, :] = sn * taper
            kept.append(squared)
        share = (VISBECK_ALPHA * 0.5**0.5) * total / (K - mixed)
        kappa = here * (BASE_DIFFUSIVITY + share)
        kap[at, :] = kappa
        weight = (0.5 * TIME_STEP) * kappa
        for k in range(K):
            cp[k, at, :] = -weight * cp[k, at, :]
            cq[k, at, :] = -weight * cq[k, at, :]
            cr[k, at, :] = (0.5 * weight) * kept[k]

    loop(physics, depth, PHYSICS)
    close(kap)

    def faces(c):
        at, up, down = (rows(c, off, FACES) for off in (0, 1, -1))
        kappa = (0.5 * TIME_STEP) * kap[at, :]
        ce[at, :] = (kappa + rolled(kappa, -1)) * me[at, :]
        cw[at, :] = (kappa + rolled(kappa, 1)) * mw[at, :]
        cn[at, :] = (kappa + (0.5 * TIME_STEP) * kap[up, :]) * mn[at, :]
        cs[at, :] = (kappa + (0.5 * TIME_STEP) * kap[down, :]) * ms[at, :]

    loop(faces, depth, FACES)

    def advance(c, source, chunk):
        at, up, down = (rows(c, off, chunk) for off in (0, 1, -1))
        mask_e, mask_w, mask_n, mask_s = (ref[at, :] for ref in (me, mw, mn, ms))
        face_e, face_w, face_n, face_s = (ref[at, :] for ref in (ce, cw, cn, cs))
        f = [source[k, at, :] for k in range(K)]
        flux, result = [], []
        for k in range(K):
            step_e = rolled(f[k], -1) - f[k]
            step_w = f[k] - rolled(f[k], 1)
            step_n = source[k, up, :] - f[k]
            step_s = f[k] - source[k, down, :]
            sum_e = mask_e * step_e + mask_w * step_w
            sum_n = mask_n * step_n + mask_s * step_s
            lateral = (face_e * step_e - face_w * step_w) + (face_n * step_n - face_s * step_s)
            drop = f[min(k + 1, K - 1)] - f[max(k - 1, 0)]
            flux.append(cp[k, at, :] * sum_e + cq[k, at, :] * sum_n + cr[k, at, :] * drop)
            result.append(f[k] + lateral)
        for k in range(K):
            if k + 1 < K:
                result[k] += flux[k + 1]
            if k > 0:
                result[k] -= flux[k - 1]
        return result

    def sweep(source, target):
        def body(c):
            result = advance(c, source, SWEEP)
            for k in range(K):
                target[k, rows(c, 0, SWEEP), :] = result[k]

        loop(body, depth, SWEEP)
        for k in range(K):
            close(target.at[k])

    for n in range(ITERS - 1):
        sweep(*((ta, tb) if n % 2 == 0 else (tb, ta)))
    source = ta if (ITERS - 1) % 2 == 0 else tb
    per_out = LANES // width

    target = tb if source is ta else ta
    chunks = depth // LAST

    inner = [lane_from(piece * g + HALO, (BR * LAST, LANES)) for g in range(SLOTS)]

    def repack(c):
        for h in range(K // per_out):
            levels = [
                rolled(target[h * per_out + m, rows(c, 0, LAST), :], width * m) for m in range(per_out)
            ]
            for g in reversed(range(SLOTS)):
                value = levels[-1]
                for m in reversed(range(per_out - 1)):
                    value = jnp.where(inner[g] < width * (m + 1), levels[m], value)
                value = rolled(value, -piece * g)
                for u in range(LAST):
                    t = owner[slot_of[c * LAST + u + depth * g]]
                    out_ref[t, h] = value[BR * u : BR * (u + 1), :]

    def final(c):
        result = advance(c, source, LAST)
        for k in range(K):
            target[k, rows(c, 0, LAST), :] = result[k]

    def last(back, carry):
        repack(chunks - back)
        final(chunks - 1 - back)
        return carry

    final(chunks - 1)
    lax.fori_loop(1, chunks, last, 0)
    repack(0)


def sweeps(order, owner, got, width):
    blocks = got.shape[0]
    depth = -(-blocks // (SLOTS * UNIT)) * UNIT
    padded = BR * (depth + 2)
    cube = pltpu.VMEM((K, padded, LANES), jnp.float32)
    flat = pltpu.VMEM((padded, LANES), jnp.float32)
    outs = K * width // LANES

    def kernel(*refs):
        sweep_kernel(width, blocks, *refs)

    return pl.pallas_call(
        kernel,
        out_shape=jax.ShapeDtypeStruct((blocks, outs, BR, LANES), jnp.float32),
        in_specs=[
            pl.BlockSpec(memory_space=pltpu.SMEM),
            pl.BlockSpec(memory_space=pltpu.SMEM),
            pl.BlockSpec(memory_space=pltpu.VMEM),
        ],
        out_specs=pl.BlockSpec(memory_space=pltpu.VMEM),
        scratch_shapes=[pltpu.SMEM((SLOTS * depth,), jnp.int32)] + [cube] * 6 + [flat] * 11,
        compiler_params=pltpu.CompilerParams(vmem_limit_bytes=40 * 1024 * 1024),
        name="sweeps",
    )(order, owner, got)


def unpack_kernel(width, got, out_ref):
    per_tile = LANES // width
    tiles = out_ref.shape[2] // LANES
    count = out_ref.shape[1] // BR
    outs = K // per_tile
    place = lane_of() // width
    for u in range(count):
        block = pl.program_id(0) * count + u
        for h in range(outs):
            for t in range(tiles):
                strips = [got[t * per_tile + q, block * outs + h] for q in range(per_tile)]
                for m in range(per_tile):
                    value = strips[-1]
                    for q in range(per_tile - 1):
                        value = jnp.where(place == (m + q) % per_tile, strips[q], value)
                    out_ref[
                        h * per_tile + m, BR * u : BR * (u + 1), LANES * t : LANES * (t + 1)
                    ] = rolled(value, -width * m)


def unpack(got, rows, columns):
    strips = got.shape[0]
    blocks = rows // BR
    width = columns // strips

    def kernel(*refs):
        unpack_kernel(width, *refs)

    return pl.pallas_call(
        kernel,
        grid=(UNPACK,),
        out_shape=jax.ShapeDtypeStruct((K, rows, columns), jnp.float32),
        in_specs=[pl.BlockSpec(memory_space=pltpu.VMEM)],
        out_specs=pl.BlockSpec((K, rows // UNPACK, columns), lambda b: (0, b, 0)),
        compiler_params=pltpu.CompilerParams(vmem_limit_bytes=SMALL),
        name="unpack",
    )(got)


def on_device(density, tracer, sea_mask, mixed_level, tile_blocks, block_owner):
    rows, columns = sea_mask.shape
    strips = lax.axis_size("gy")
    ring = lax.axis_size("gx")
    width = columns // strips
    blocks = rows // BR
    planes = jnp.concatenate([density, tracer])
    near, far = edges(planes, sea_mask, mixed_level)
    near = lax.ppermute(near, "gx", [(i, i ^ 1) for i in range(ring)])
    far = lax.ppermute(far, "gx", [(i, (((i + 1) ^ 1) - 1) % ring) for i in range(ring)])
    packed = pack(planes, sea_mask, mixed_level, strips)
    packed = patch(near, far, packed, width)
    got = lax.all_to_all(packed, "gy", split_axis=0, concat_axis=0, tiled=True)
    done = sweeps(tile_blocks, block_owner, got.reshape(strips * blocks, VREGS, BR, LANES), width)
    back = lax.all_to_all(
        done.reshape(strips, -1, BR, LANES), "gy", split_axis=0, concat_axis=0, tiled=True
    )
    return unpack(back, rows, columns)


def solution(mesh):
    placed = (P(None, "gy", "gx"), P(None, "gy", "gx"), P("gy", "gx"), P("gy", "gx"), P(), P())
    return jax.shard_map(
        on_device, mesh=mesh, in_specs=placed, out_specs=P(None, "gy", "gx"), check_vma=False
    )
```

```python
import jax
import jax.numpy as jnp
from jax import lax
from jax.experimental import pallas as pl
from jax.experimental.pallas import tpu as pltpu
from jax.sharding import PartitionSpec as P

K = 8
BR = 8
ITERS = 4
HALO = ITERS + 1
LANES = 128
SLOTS = 3
VREGS = 6
UNPACK = 2
SMALL = 12 * 1024 * 1024
PLANES = 2 * K + 2
UNIT = 4
DEEPEST = 4
GATHER = 4
FACES = 22
SWEEP = 4
LAST = 4

TIME_STEP = 0.2
STRATIFICATION = 1.0
DENSITY_FLOOR = 0.25
SLOPE_LIMIT = 1.0
TAPER_WIDTH = 0.5
KERNEL_OFFSET = 0.05
BASE_DIFFUSIVITY = 0.2
VISBECK_ALPHA = 0.5


def rolled(x, shift):
    shift %= LANES
    return x if shift == 0 else pltpu.roll(x, shift, x.ndim - 1)


def lane_of(shape=(BR, LANES)):
    return lax.broadcasted_iota(jnp.int32, shape, len(shape) - 1)


def plane_at(register, piece):
    if piece == 2 and register == 2:
        return 2 * K
    if piece == 2 and register == 5:
        return 2 * K + 1
    return register % 3 + 3 * piece + (K if register >= 3 else 0)


def plane_of(planes, mask, mixed, p, rows, columns):
    if p < 2 * K:
        return planes[p, rows, columns]
    return (mask if p == 2 * K else mixed)[rows, columns].astype(jnp.float32)


def edges_kernel(planes, mask, mixed, near_ref, far_ref):
    shape = near_ref.shape
    lane = lane_of(shape)
    last = planes.shape[2] - LANES
    sides = []
    for start, edge in ((0, 0), (last, LANES - HALO)):
        out = jnp.zeros(shape, jnp.float32)
        for p in range(PLANES):
            at = HALO * p
            plane = plane_of(planes, mask, mixed, p, slice(None), slice(start, start + LANES))
            plane = rolled(plane, at - edge)
            out = jnp.where((lane >= at) & (lane < at + HALO), plane, out)
        sides.append(out)
    head, tail = sides
    even = lax.axis_index("gx") % 2 == 0
    near_ref[...] = jnp.where(even, tail, head)
    far_ref[...] = jnp.where(even, head, tail)


def edges(planes, mask, mixed):
    whole = pl.BlockSpec(memory_space=pltpu.VMEM)
    out = jax.ShapeDtypeStruct((planes.shape[1], LANES), jnp.float32)
    return pl.pallas_call(
        edges_kernel,
        out_shape=(out, out),
        in_specs=[whole, whole, whole],
        out_specs=(whole, whole),
        compiler_params=pltpu.CompilerParams(vmem_limit_bytes=SMALL),
        name="edges",
    )(planes, mask, mixed)


def pack_kernel(width, planes, mask, mixed, out_ref):
    piece = width + 2 * HALO
    per_tile = LANES // width
    tiles = planes.shape[2] // LANES
    lane = lane_of()

    def below(limit, start):
        return ((lane - start) & (LANES - 1)) < limit

    west_half = [below(LANES // 2, piece * m) for m in range(SLOTS)]
    one = [below(piece, width * q - HALO) for q in range(per_tile)]
    two = [below(2 * piece, width * q - HALO) for q in range(per_tile)]

    for b in range(planes.shape[1] // BR):
        for v in range(VREGS):
            whole, seam = [], []
            for m in range(SLOTS):
                own = [
                    rolled(
                        plane_of(
                            planes,
                            mask,
                            mixed,
                            plane_at(v, m),
                            slice(BR * b, BR * (b + 1)),
                            slice(LANES * t, LANES * (t + 1)),
                        ),
                        piece * m,
                    )
                    for t in range(tiles)
                ]
                whole.append(own)
                seam.append(
                    [own[0]]
                    + [jnp.where(west_half[m], own[t], own[t - 1]) for t in range(1, tiles)]
                    + [own[-1]]
                )
            for j in range(tiles * per_tile):
                t, q = divmod(j, per_tile)
                if q == 0:
                    parts = [seam[m][t] for m in range(SLOTS)]
                elif q == per_tile - 1:
                    parts = [seam[m][t + 1] for m in range(SLOTS)]
                else:
                    parts = [whole[m][t] for m in range(SLOTS)]
                out_ref[j, b * VREGS + v] = jnp.where(one[q], parts[0], jnp.where(two[q], parts[1], parts[2]))


def pack(planes, mask, mixed, strips):
    rows, columns = planes.shape[1:]
    whole = pl.BlockSpec(memory_space=pltpu.VMEM)
    width = columns // strips

    def kernel(*refs):
        pack_kernel(width, *refs)

    return pl.pallas_call(
        kernel,
        out_shape=jax.ShapeDtypeStruct((strips, rows // BR * VREGS, BR, LANES), jnp.float32),
        in_specs=[whole, whole, whole],
        out_specs=whole,
        compiler_params=pltpu.CompilerParams(vmem_limit_bytes=SMALL),
        cost_estimate=pl.CostEstimate(flops=20000000, bytes_accessed=6000000, transcendentals=0),
        name="pack",
    )(planes, mask, mixed)


def patch_kernel(width, near, far, packed, out_ref):
    piece = width + 2 * HALO
    even = lax.axis_index("gx") % 2 == 0
    lane = lane_of()
    strips = packed.shape[0]

    def fill(b, strip, evens, odds, start):
        here = slice(BR * b, BR * (b + 1))
        rim = jnp.where(even, evens[here, :], odds[here, :])
        for v in range(VREGS):
            value = packed[strip, b * VREGS + v]
            for m in range(SLOTS):
                at = (piece * m + start) % LANES
                here = (lane >= at) & (lane < at + HALO)
                value = jnp.where(here, rolled(rim, at - HALO * plane_at(v, m)), value)
            out_ref[strip, b * VREGS + v] = value

    for b in range(near.shape[0] // BR):
        fill(b, 0, far, near, LANES - HALO)
        fill(b, strips - 1, near, far, 0)


def patch(near, far, packed, width):
    whole = pl.BlockSpec(memory_space=pltpu.VMEM)

    def kernel(*refs):
        patch_kernel(width, *refs)

    return pl.pallas_call(
        kernel,
        out_shape=jax.ShapeDtypeStruct(packed.shape, jnp.float32),
        in_specs=[whole, whole, whole],
        out_specs=whole,
        input_output_aliases={2: 0},
        compiler_params=pltpu.CompilerParams(vmem_limit_bytes=SMALL),
        name="patch",
    )(near, far, packed)


def sweep_kernel(
    width, blocks, order, owner, got, out_ref, slot_of, rho, ta, tb, cp, cq, cr, sea, mix, kap, me, mw, mn, ms, ce, cw, cn, cs
):
    piece = width + 2 * HALO
    depth = (sea.shape[0] - 2 * BR) // BR
    strip = lax.axis_index("gy") % (LANES // width)

    def lane_from(start, shape=(BR, LANES)):
        return (lane_of(shape) - (width * strip + (start - HALO))) & (LANES - 1)

    lane = lane_from(0)
    first = lane < piece
    second = lane < 2 * piece

    def invert(s, carry):
        slot_of[order[s]] = s
        return carry

    lax.fori_loop(0, blocks, invert, 0, unroll=8)
    for b in range(blocks, SLOTS * depth):
        slot_of[b] = slot_of[0]

    def loop(body, count, chunk):
        def some(i, carry):
            body(i)
            return carry

        lax.fori_loop(0, count // chunk, some, 0)

    def rows(c, off=0, chunk=1):
        start = BR + BR * chunk * c
        if off == 0:
            return pl.ds(pl.multiple_of(start, BR), BR * chunk)
        return pl.ds(start + off, BR * chunk)

    def close(ref):
        top = jnp.where(first, 0.0, rolled(ref[pl.ds(BR * depth, BR), :], piece))
        bottom = jnp.where(second, rolled(ref[pl.ds(BR, BR), :], -piece), 0.0)
        ref[pl.ds(0, BR), :] = top
        ref[pl.ds(BR * (depth + 1), BR), :] = bottom

    def gather(c):
        for u in range(GATHER):
            i = c * GATHER + u
            slots = [slot_of[i + depth * m] for m in range(SLOTS)]
            owners = [owner[s] for s in slots]
            real = jnp.where(i + depth * (SLOTS - 1) < blocks, 1.0, 0.0)
            at = rows(i)
            for v in range(VREGS):
                where = slots if v < 3 else owners
                parts = [got[where[m], v] for m in range(SLOTS)]
                parts[2] = parts[2] * real
                for n in range(SLOTS):
                    moved = [rolled(parts[m], piece * (m - n)) for m in range(SLOTS)]
                    plane = jnp.where(first, moved[0], jnp.where(second, moved[1], moved[2]))
                    p = plane_at(v, n)
                    if p < K:
                        rho[p, at, :] = plane
                    elif p < 2 * K:
                        ta[p - K, at, :] = plane
                    elif p == 2 * K:
                        sea[at, :] = plane
            levels = [got[slots[m], 5] for m in range(SLOTS)]
            levels[2] = levels[2] * real
            levels = [rolled(levels[m], piece * (m - 2)) for m in range(SLOTS)]
            mix[at, :] = jnp.where(first, levels[0], jnp.where(second, levels[1], levels[2]))

    def physics(c):
        at, up, down = (rows(c, off, GATHER) for off in (0, 1, -1))
        mixed = mix[at, :]
        here = sea[at, :]
        east = rolled(here, -1) * here
        west = rolled(here, 1) * here
        north = sea[up, :] * here
        south = sea[down, :] * here
        me[at, :] = east
        mw[at, :] = west
        mn[at, :] = north
        ms[at, :] = south
        per_mixed = 1.0 / (mixed + 1.0)
        f = [rho[k, at, :] for k in range(K)]
        total = jnp.zeros_like(here)
        kept = []
        for k in range(K):
            sum_e = east * (rolled(f[k], -1) - f[k]) + west * (f[k] - rolled(f[k], 1))
            sum_n = north * (rho[k, up, :] - f[k]) + south * (f[k] - rho[k, down, :])
            above, under = max(k - 1, 0), min(k + 1, K - 1)
            rising = STRATIFICATION * (under - above)
            twice = jnp.maximum((f[under] - f[above]) + rising, 2.0 * DENSITY_FLOOR)
            scale = 1.0 / twice
            se = sum_e * scale
            sn = sum_n * scale
            squared = se * se + sn * sn
            taper = 0.5 + 0.5 * jnp.tanh(SLOPE_LIMIT / TAPER_WIDTH - squared * (1.0 / TAPER_WIDTH))
            if k < DEEPEST:
                taper = taper * jnp.minimum(1.0, (k + 1.0) * per_mixed)
            squared = squared * (taper * taper)
            under_root = twice * (squared + KERNEL_OFFSET)
            root = under_root * lax.rsqrt(under_root)
            total += jnp.where(mixed <= float(k), root, 0.0) if k < DEEPEST else root
            cp[k, at, :] = se * taper
            cq[k, at, :] = sn * taper
            kept.append(squared)
        share = (VISBECK_ALPHA * 0.5**0.5) * total / (K - mixed)
        kappa = here * (BASE_DIFFUSIVITY + share)
        kap[at, :] = kappa
        weight = (0.5 * TIME_STEP) * kappa
        for k in range(K):
            cp[k, at, :] = -weight * cp[k, at, :]
            cq[k, at, :] = -weight * cq[k, at, :]
            cr[k, at, :] = (0.5 * weight) * kept[k]

    chunks = depth // GATHER

    def opening(i, carry):
        gather((i + chunks - 1) % chunks)
        return carry

    def both(c, carry):
        physics(c)
        gather(c + 2)
        return carry

    def closing(c, carry):
        physics(c)
        return carry

    lax.fori_loop(0, 3, opening, 0)
    for k in range(K):
        close(rho.at[k])
    close(sea)
    lax.fori_loop(0, chunks - 3, both, 0)
    lax.fori_loop(chunks - 3, chunks, closing, 0)
    for k in range(K):
        close(ta.at[k])
    close(kap)

    def faces(c):
        at, up, down = (rows(c, off, FACES) for off in (0, 1, -1))
        kappa = (0.5 * TIME_STEP) * kap[at, :]
        ce[at, :] = (kappa + rolled(kappa, -1)) * me[at, :]
        cw[at, :] = (kappa + rolled(kappa, 1)) * mw[at, :]
        cn[at, :] = (kappa + (0.5 * TIME_STEP) * kap[up, :]) * mn[at, :]
        cs[at, :] = (kappa + (0.5 * TIME_STEP) * kap[down, :]) * ms[at, :]

    loop(faces, depth, FACES)

    def advance(c, source, chunk):
        at, up, down = (rows(c, off, chunk) for off in (0, 1, -1))
        mask_e, mask_w, mask_n, mask_s = (ref[at, :] for ref in (me, mw, mn, ms))
        face_e, face_w, face_n, face_s = (ref[at, :] for ref in (ce, cw, cn, cs))
        f = [source[k, at, :] for k in range(K)]
        flux, result = [], []
        for k in range(K):
            step_e = rolled(f[k], -1) - f[k]
            step_w = f[k] - rolled(f[k], 1)
            step_n = source[k, up, :] - f[k]
            step_s = f[k] - source[k, down, :]
            sum_e = mask_e * step_e + mask_w * step_w
            sum_n = mask_n * step_n + mask_s * step_s
            lateral = (face_e * step_e - face_w * step_w) + (face_n * step_n - face_s * step_s)
            drop = f[min(k + 1, K - 1)] - f[max(k - 1, 0)]
            flux.append(cp[k, at, :] * sum_e + cq[k, at, :] * sum_n + cr[k, at, :] * drop)
            result.append(f[k] + lateral)
        for k in range(K):
            if k + 1 < K:
                result[k] += flux[k + 1]
            if k > 0:
                result[k] -= flux[k - 1]
        return result

    def sweep(source, target):
        def body(c):
            result = advance(c, source, SWEEP)
            for k in range(K):
                target[k, rows(c, 0, SWEEP), :] = result[k]

        loop(body, depth, SWEEP)
        for k in range(K):
            close(target.at[k])

    for n in range(ITERS - 1):
        sweep(*((ta, tb) if n % 2 == 0 else (tb, ta)))
    source = ta if (ITERS - 1) % 2 == 0 else tb
    per_out = LANES // width

    target = tb if source is ta else ta
    chunks = depth // LAST

    inner = [lane_from(piece * g + HALO, (BR * LAST, LANES)) for g in range(SLOTS)]

    def repack(c):
        for h in range(K // per_out):
            levels = [
                rolled(target[h * per_out + m, rows(c, 0, LAST), :], width * m) for m in range(per_out)
            ]
            for g in reversed(range(SLOTS)):
                value = levels[-1]
                for m in reversed(range(per_out - 1)):
                    value = jnp.where(inner[g] < width * (m + 1), levels[m], value)
                value = rolled(value, -piece * g)
                for u in range(LAST):
                    t = owner[slot_of[c * LAST + u + depth * g]]
                    out_ref[t, h] = value[BR * u : BR * (u + 1), :]

    def final(c):
        result = advance(c, source, LAST)
        for k in range(K):
            target[k, rows(c, 0, LAST), :] = result[k]

    def last(back, carry):
        repack(chunks - back)
        final(chunks - 1 - back)
        return carry

    final(chunks - 1)
    lax.fori_loop(1, chunks, last, 0)
    repack(0)


def sweeps(order, owner, got, width):
    blocks = got.shape[0]
    depth = -(-blocks // (SLOTS * UNIT)) * UNIT
    padded = BR * (depth + 2)
    cube = pltpu.VMEM((K, padded, LANES), jnp.float32)
    flat = pltpu.VMEM((padded, LANES), jnp.float32)
    outs = K * width // LANES

    def kernel(*refs):
        sweep_kernel(width, blocks, *refs)

    return pl.pallas_call(
        kernel,
        out_shape=jax.ShapeDtypeStruct((blocks, outs, BR, LANES), jnp.float32),
        in_specs=[
            pl.BlockSpec(memory_space=pltpu.SMEM),
            pl.BlockSpec(memory_space=pltpu.SMEM),
            pl.BlockSpec(memory_space=pltpu.VMEM),
        ],
        out_specs=pl.BlockSpec(memory_space=pltpu.VMEM),
        scratch_shapes=[pltpu.SMEM((SLOTS * depth,), jnp.int32)] + [cube] * 6 + [flat] * 11,
        compiler_params=pltpu.CompilerParams(vmem_limit_bytes=40 * 1024 * 1024),
        name="sweeps",
    )(order, owner, got)


def unpack_kernel(width, got, out_ref):
    per_tile = LANES // width
    tiles = out_ref.shape[2] // LANES
    count = out_ref.shape[1] // BR
    outs = K // per_tile
    place = lane_of() // width
    for u in range(count):
        block = pl.program_id(0) * count + u
        for h in range(outs):
            for t in range(tiles):
                strips = [got[t * per_tile + q, block * outs + h] for q in range(per_tile)]
                for m in range(per_tile):
                    value = strips[-1]
                    for q in range(per_tile - 1):
                        value = jnp.where(place == (m + q) % per_tile, strips[q], value)
                    out_ref[
                        h * per_tile + m, BR * u : BR * (u + 1), LANES * t : LANES * (t + 1)
                    ] = rolled(value, -width * m)


def unpack(got, rows, columns):
    strips = got.shape[0]
    blocks = rows // BR
    width = columns // strips

    def kernel(*refs):
        unpack_kernel(width, *refs)

    return pl.pallas_call(
        kernel,
        grid=(UNPACK,),
        out_shape=jax.ShapeDtypeStruct((K, rows, columns), jnp.float32),
        in_specs=[pl.BlockSpec(memory_space=pltpu.VMEM)],
        out_specs=pl.BlockSpec((K, rows // UNPACK, columns), lambda b: (0, b, 0)),
        compiler_params=pltpu.CompilerParams(vmem_limit_bytes=SMALL),
        name="unpack",
    )(got)


def on_device(density, tracer, sea_mask, mixed_level, tile_blocks, block_owner):
    rows, columns = sea_mask.shape
    strips = lax.axis_size("gy")
    ring = lax.axis_size("gx")
    width = columns // strips
    blocks = rows // BR
    planes = jnp.concatenate([density, tracer])
    near, far = edges(planes, sea_mask, mixed_level)
    near = lax.ppermute(near, "gx", [(i, i ^ 1) for i in range(ring)])
    far = lax.ppermute(far, "gx", [(i, (((i + 1) ^ 1) - 1) % ring) for i in range(ring)])
    packed = pack(planes, sea_mask, mixed_level, strips)
    packed = patch(near, far, packed, width)
    got = lax.all_to_all(packed, "gy", split_axis=0, concat_axis=0, tiled=True)
    done = sweeps(tile_blocks, block_owner, got.reshape(strips * blocks, VREGS, BR, LANES), width)
    back = lax.all_to_all(
        done.reshape(strips, -1, BR, LANES), "gy", split_axis=0, concat_axis=0, tiled=True
    )
    return unpack(back, rows, columns)


def solution(mesh):
    placed = (P(None, "gy", "gx"), P(None, "gy", "gx"), P("gy", "gx"), P("gy", "gx"), P(), P())
    return jax.shard_map(
        on_device, mesh=mesh, in_specs=placed, out_specs=P(None, "gy", "gx"), check_vma=False
    )
```

```python
import jax
import jax.numpy as jnp
from jax import lax
from jax.experimental import pallas as pl
from jax.experimental.pallas import tpu as pltpu
from jax.sharding import PartitionSpec as P

K = 8
BR = 8
ITERS = 4
HALO = ITERS + 1
LANES = 128
SLOTS = 3
VREGS = 6
UNPACK = 2
SMALL = 12 * 1024 * 1024
PLANES = 2 * K + 2
UNIT = 4
DEEPEST = 4
GATHER = 4
FACES = 44
SWEEP = 4
LAST = 4

TIME_STEP = 0.2
STRATIFICATION = 1.0
DENSITY_FLOOR = 0.25
SLOPE_LIMIT = 1.0
TAPER_WIDTH = 0.5
KERNEL_OFFSET = 0.05
BASE_DIFFUSIVITY = 0.2
VISBECK_ALPHA = 0.5


def rolled(x, shift):
    shift %= LANES
    return x if shift == 0 else pltpu.roll(x, shift, x.ndim - 1)


def lane_of(shape=(BR, LANES)):
    return lax.broadcasted_iota(jnp.int32, shape, len(shape) - 1)


def plane_at(register, piece):
    if piece == 2 and register == 2:
        return 2 * K
    if piece == 2 and register == 5:
        return 2 * K + 1
    return register % 3 + 3 * piece + (K if register >= 3 else 0)


def plane_of(planes, mask, mixed, p, rows, columns):
    if p < 2 * K:
        return planes[p, rows, columns]
    return (mask if p == 2 * K else mixed)[rows, columns].astype(jnp.float32)


def edges_kernel(planes, mask, mixed, near_ref, far_ref):
    shape = near_ref.shape
    lane = lane_of(shape)
    last = planes.shape[2] - LANES
    sides = []
    for start, edge in ((0, 0), (last, LANES - HALO)):
        out = jnp.zeros(shape, jnp.float32)
        for p in range(PLANES):
            at = HALO * p
            plane = plane_of(planes, mask, mixed, p, slice(None), slice(start, start + LANES))
            plane = rolled(plane, at - edge)
            out = jnp.where((lane >= at) & (lane < at + HALO), plane, out)
        sides.append(out)
    head, tail = sides
    even = lax.axis_index("gx") % 2 == 0
    near_ref[...] = jnp.where(even, tail, head)
    far_ref[...] = jnp.where(even, head, tail)


def edges(planes, mask, mixed):
    whole = pl.BlockSpec(memory_space=pltpu.VMEM)
    out = jax.ShapeDtypeStruct((planes.shape[1], LANES), jnp.float32)
    return pl.pallas_call(
        edges_kernel,
        out_shape=(out, out),
        in_specs=[whole, whole, whole],
        out_specs=(whole, whole),
        compiler_params=pltpu.CompilerParams(vmem_limit_bytes=SMALL),
        name="edges",
    )(planes, mask, mixed)


def pack_kernel(width, planes, mask, mixed, out_ref):
    piece = width + 2 * HALO
    per_tile = LANES // width
    tiles = planes.shape[2] // LANES
    lane = lane_of()

    def below(limit, start):
        return ((lane - start) & (LANES - 1)) < limit

    west_half = [below(LANES // 2, piece * m) for m in range(SLOTS)]
    one = [below(piece, width * q - HALO) for q in range(per_tile)]
    two = [below(2 * piece, width * q - HALO) for q in range(per_tile)]

    for b in range(planes.shape[1] // BR):
        for v in range(VREGS):
            whole, seam = [], []
            for m in range(SLOTS):
                own = [
                    rolled(
                        plane_of(
                            planes,
                            mask,
                            mixed,
                            plane_at(v, m),
                            slice(BR * b, BR * (b + 1)),
                            slice(LANES * t, LANES * (t + 1)),
                        ),
                        piece * m,
                    )
                    for t in range(tiles)
                ]
                whole.append(own)
                seam.append(
                    [own[0]]
                    + [jnp.where(west_half[m], own[t], own[t - 1]) for t in range(1, tiles)]
                    + [own[-1]]
                )
            for j in range(tiles * per_tile):
                t, q = divmod(j, per_tile)
                if q == 0:
                    parts = [seam[m][t] for m in range(SLOTS)]
                elif q == per_tile - 1:
                    parts = [seam[m][t + 1] for m in range(SLOTS)]
                else:
                    parts = [whole[m][t] for m in range(SLOTS)]
                out_ref[j, b * VREGS + v] = jnp.where(one[q], parts[0], jnp.where(two[q], parts[1], parts[2]))


def pack(planes, mask, mixed, strips):
    rows, columns = planes.shape[1:]
    whole = pl.BlockSpec(memory_space=pltpu.VMEM)
    width = columns // strips

    def kernel(*refs):
        pack_kernel(width, *refs)

    return pl.pallas_call(
        kernel,
        out_shape=jax.ShapeDtypeStruct((strips, rows // BR * VREGS, BR, LANES), jnp.float32),
        in_specs=[whole, whole, whole],
        out_specs=whole,
        compiler_params=pltpu.CompilerParams(vmem_limit_bytes=SMALL),
        cost_estimate=pl.CostEstimate(flops=20000000, bytes_accessed=6000000, transcendentals=0),
        name="pack",
    )(planes, mask, mixed)


def patch_kernel(width, near, far, packed, out_ref):
    piece = width + 2 * HALO
    even = lax.axis_index("gx") % 2 == 0
    lane = lane_of()
    strips = packed.shape[0]

    def fill(b, strip, evens, odds, start):
        here = slice(BR * b, BR * (b + 1))
        rim = jnp.where(even, evens[here, :], odds[here, :])
        for v in range(VREGS):
            value = packed[strip, b * VREGS + v]
            for m in range(SLOTS):
                at = (piece * m + start) % LANES
                here = (lane >= at) & (lane < at + HALO)
                value = jnp.where(here, rolled(rim, at - HALO * plane_at(v, m)), value)
            out_ref[strip, b * VREGS + v] = value

    for b in range(near.shape[0] // BR):
        fill(b, 0, far, near, LANES - HALO)
        fill(b, strips - 1, near, far, 0)


def patch(near, far, packed, width):
    whole = pl.BlockSpec(memory_space=pltpu.VMEM)

    def kernel(*refs):
        patch_kernel(width, *refs)

    return pl.pallas_call(
        kernel,
        out_shape=jax.ShapeDtypeStruct(packed.shape, jnp.float32),
        in_specs=[whole, whole, whole],
        out_specs=whole,
        input_output_aliases={2: 0},
        compiler_params=pltpu.CompilerParams(vmem_limit_bytes=SMALL),
        name="patch",
    )(near, far, packed)


def sweep_kernel(
    width, blocks, order, owner, got, out_ref, slot_of, rho, ta, tb, cp, cq, cr, sea, mix, kap, me, mw, mn, ms, ce, cw, cn, cs
):
    piece = width + 2 * HALO
    depth = (sea.shape[0] - 2 * BR) // BR
    strip = lax.axis_index("gy") % (LANES // width)

    def lane_from(start, shape=(BR, LANES)):
        return (lane_of(shape) - (width * strip + (start - HALO))) & (LANES - 1)

    lane = lane_from(0)
    first = lane < piece
    second = lane < 2 * piece

    def invert(s, carry):
        slot_of[order[s]] = s
        return carry

    lax.fori_loop(0, blocks, invert, 0, unroll=8)
    for b in range(blocks, SLOTS * depth):
        slot_of[b] = slot_of[0]

    def loop(body, count, chunk):
        def some(i, carry):
            body(i)
            return carry

        lax.fori_loop(0, count // chunk, some, 0)

    def rows(c, off=0, chunk=1):
        start = BR + BR * chunk * c
        if off == 0:
            return pl.ds(pl.multiple_of(start, BR), BR * chunk)
        return pl.ds(start + off, BR * chunk)

    def close(ref):
        top = jnp.where(first, 0.0, rolled(ref[pl.ds(BR * depth, BR), :], piece))
        bottom = jnp.where(second, rolled(ref[pl.ds(BR, BR), :], -piece), 0.0)
        ref[pl.ds(0, BR), :] = top
        ref[pl.ds(BR * (depth + 1), BR), :] = bottom

    def gather(c):
        for u in range(GATHER):
            i = c * GATHER + u
            slots = [slot_of[i + depth * m] for m in range(SLOTS)]
            owners = [owner[s] for s in slots]
            real = jnp.where(i + depth * (SLOTS - 1) < blocks, 1.0, 0.0)
            at = rows(i)
            for v in range(VREGS):
                where = slots if v < 3 else owners
                parts = [got[where[m], v] for m in range(SLOTS)]
                parts[2] = parts[2] * real
                for n in range(SLOTS):
                    moved = [rolled(parts[m], piece * (m - n)) for m in range(SLOTS)]
                    plane = jnp.where(first, moved[0], jnp.where(second, moved[1], moved[2]))
                    p = plane_at(v, n)
                    if p < K:
                        rho[p, at, :] = plane
                    elif p < 2 * K:
                        ta[p - K, at, :] = plane
                    elif p == 2 * K:
                        sea[at, :] = plane
            levels = [got[slots[m], 5] for m in range(SLOTS)]
            levels[2] = levels[2] * real
            levels = [rolled(levels[m], piece * (m - 2)) for m in range(SLOTS)]
            mix[at, :] = jnp.where(first, levels[0], jnp.where(second, levels[1], levels[2]))

    def physics(c):
        at, up, down = (rows(c, off, GATHER) for off in (0, 1, -1))
        mixed = mix[at, :]
        here = sea[at, :]
        east = rolled(here, -1) * here
        west = rolled(here, 1) * here
        north = sea[up, :] * here
        south = sea[down, :] * here
        me[at, :] = east
        mw[at, :] = west
        mn[at, :] = north
        ms[at, :] = south
        per_mixed = 1.0 / (mixed + 1.0)
        f = [rho[k, at, :] for k in range(K)]
        total = jnp.zeros_like(here)
        kept = []
        for k in range(K):
            sum_e = east * (rolled(f[k], -1) - f[k]) + west * (f[k] - rolled(f[k], 1))
            sum_n = north * (rho[k, up, :] - f[k]) + south * (f[k] - rho[k, down, :])
            above, under = max(k - 1, 0), min(k + 1, K - 1)
            rising = STRATIFICATION * (under - above)
            twice = jnp.maximum((f[under] - f[above]) + rising, 2.0 * DENSITY_FLOOR)
            scale = 1.0 / twice
            se = sum_e * scale
            sn = sum_n * scale
            squared = se * se + sn * sn
            taper = 0.5 + 0.5 * jnp.tanh(SLOPE_LIMIT / TAPER_WIDTH - squared * (1.0 / TAPER_WIDTH))
            if k < DEEPEST:
                taper = taper * jnp.minimum(1.0, (k + 1.0) * per_mixed)
            squared = squared * (taper * taper)
            under_root = twice * (squared + KERNEL_OFFSET)
            root = under_root * lax.rsqrt(under_root)
            total += jnp.where(mixed <= float(k), root, 0.0) if k < DEEPEST else root
            cp[k, at, :] = se * taper
            cq[k, at, :] = sn * taper
            kept.append(squared)
        share = (VISBECK_ALPHA * 0.5**0.5) * total / (K - mixed)
        kappa = here * (BASE_DIFFUSIVITY + share)
        kap[at, :] = kappa
        weight = (0.5 * TIME_STEP) * kappa
        for k in range(K):
            cp[k, at, :] = -weight * cp[k, at, :]
            cq[k, at, :] = -weight * cq[k, at, :]
            cr[k, at, :] = (0.5 * weight) * kept[k]

    chunks = depth // GATHER

    def opening(i, carry):
        gather((i + chunks - 1) % chunks)
        return carry

    def both(c, carry):
        physics(c)
        gather(c + 2)
        return carry

    def closing(c, carry):
        physics(c)
        return carry

    lax.fori_loop(0, 3, opening, 0)
    for k in range(K):
        close(rho.at[k])
    close(sea)
    lax.fori_loop(0, chunks - 3, both, 0)
    lax.fori_loop(chunks - 3, chunks, closing, 0)
    for k in range(K):
        close(ta.at[k])
    close(kap)

    def faces(c):
        at, up, down = (rows(c, off, FACES) for off in (0, 1, -1))
        kappa = (0.5 * TIME_STEP) * kap[at, :]
        ce[at, :] = (kappa + rolled(kappa, -1)) * me[at, :]
        cw[at, :] = (kappa + rolled(kappa, 1)) * mw[at, :]
        cn[at, :] = (kappa + (0.5 * TIME_STEP) * kap[up, :]) * mn[at, :]
        cs[at, :] = (kappa + (0.5 * TIME_STEP) * kap[down, :]) * ms[at, :]

    loop(faces, depth, FACES)

    def advance(c, source, chunk):
        at, up, down = (rows(c, off, chunk) for off in (0, 1, -1))
        mask_e, mask_w, mask_n, mask_s = (ref[at, :] for ref in (me, mw, mn, ms))
        face_e, face_w, face_n, face_s = (ref[at, :] for ref in (ce, cw, cn, cs))
        f = [source[k, at, :] for k in range(K)]
        flux, result = [], []
        for k in range(K):
            step_e = rolled(f[k], -1) - f[k]
            step_w = f[k] - rolled(f[k], 1)
            step_n = source[k, up, :] - f[k]
            step_s = f[k] - source[k, down, :]
            sum_e = mask_e * step_e + mask_w * step_w
            sum_n = mask_n * step_n + mask_s * step_s
            lateral = (face_e * step_e - face_w * step_w) + (face_n * step_n - face_s * step_s)
            drop = f[min(k + 1, K - 1)] - f[max(k - 1, 0)]
            flux.append(cp[k, at, :] * sum_e + cq[k, at, :] * sum_n + cr[k, at, :] * drop)
            result.append(f[k] + lateral)
        for k in range(K):
            if k + 1 < K:
                result[k] += flux[k + 1]
            if k > 0:
                result[k] -= flux[k - 1]
        return result

    def sweep(source, target):
        def body(c):
            result = advance(c, source, SWEEP)
            for k in range(K):
                target[k, rows(c, 0, SWEEP), :] = result[k]

        loop(body, depth, SWEEP)
        for k in range(K):
            close(target.at[k])

    for n in range(ITERS - 1):
        sweep(*((ta, tb) if n % 2 == 0 else (tb, ta)))
    source = ta if (ITERS - 1) % 2 == 0 else tb
    per_out = LANES // width

    target = tb if source is ta else ta
    chunks = depth // LAST

    inner = [lane_from(piece * g + HALO, (BR * LAST, LANES)) for g in range(SLOTS)]

    def repack(c):
        for h in range(K // per_out):
            levels = [
                rolled(target[h * per_out + m, rows(c, 0, LAST), :], width * m) for m in range(per_out)
            ]
            for g in reversed(range(SLOTS)):
                value = levels[-1]
                for m in reversed(range(per_out - 1)):
                    value = jnp.where(inner[g] < width * (m + 1), levels[m], value)
                value = rolled(value, -piece * g)
                for u in range(LAST):
                    t = owner[slot_of[c * LAST + u + depth * g]]
                    out_ref[t, h] = value[BR * u : BR * (u + 1), :]

    def final(c):
        result = advance(c, source, LAST)
        for k in range(K):
            target[k, rows(c, 0, LAST), :] = result[k]

    def last(back, carry):
        repack(chunks - back)
        final(chunks - 1 - back)
        return carry

    final(chunks - 1)
    lax.fori_loop(1, chunks, last, 0)
    repack(0)


def sweeps(order, owner, got, width):
    blocks = got.shape[0]
    depth = -(-blocks // (SLOTS * UNIT)) * UNIT
    padded = BR * (depth + 2)
    cube = pltpu.VMEM((K, padded, LANES), jnp.float32)
    flat = pltpu.VMEM((padded, LANES), jnp.float32)
    outs = K * width // LANES

    def kernel(*refs):
        sweep_kernel(width, blocks, *refs)

    return pl.pallas_call(
        kernel,
        out_shape=jax.ShapeDtypeStruct((blocks, outs, BR, LANES), jnp.float32),
        in_specs=[
            pl.BlockSpec(memory_space=pltpu.SMEM),
            pl.BlockSpec(memory_space=pltpu.SMEM),
            pl.BlockSpec(memory_space=pltpu.VMEM),
        ],
        out_specs=pl.BlockSpec(memory_space=pltpu.VMEM),
        scratch_shapes=[pltpu.SMEM((SLOTS * depth,), jnp.int32)] + [cube] * 6 + [flat] * 11,
        compiler_params=pltpu.CompilerParams(vmem_limit_bytes=40 * 1024 * 1024),
        name="sweeps",
    )(order, owner, got)


def unpack_kernel(width, got, out_ref):
    per_tile = LANES // width
    tiles = out_ref.shape[2] // LANES
    count = out_ref.shape[1] // BR
    outs = K // per_tile
    place = lane_of() // width
    for u in range(count):
        block = pl.program_id(0) * count + u
        for h in range(outs):
            for t in range(tiles):
                strips = [got[t * per_tile + q, block * outs + h] for q in range(per_tile)]
                for m in range(per_tile):
                    value = strips[-1]
                    for q in range(per_tile - 1):
                        value = jnp.where(place == (m + q) % per_tile, strips[q], value)
                    out_ref[
                        h * per_tile + m, BR * u : BR * (u + 1), LANES * t : LANES * (t + 1)
                    ] = rolled(value, -width * m)


def unpack(got, rows, columns):
    strips = got.shape[0]
    blocks = rows // BR
    width = columns // strips

    def kernel(*refs):
        unpack_kernel(width, *refs)

    return pl.pallas_call(
        kernel,
        grid=(UNPACK,),
        out_shape=jax.ShapeDtypeStruct((K, rows, columns), jnp.float32),
        in_specs=[pl.BlockSpec(memory_space=pltpu.VMEM)],
        out_specs=pl.BlockSpec((K, rows // UNPACK, columns), lambda b: (0, b, 0)),
        compiler_params=pltpu.CompilerParams(vmem_limit_bytes=SMALL),
        name="unpack",
    )(got)


def on_device(density, tracer, sea_mask, mixed_level, tile_blocks, block_owner):
    rows, columns = sea_mask.shape
    strips = lax.axis_size("gy")
    ring = lax.axis_size("gx")
    width = columns // strips
    blocks = rows // BR
    planes = jnp.concatenate([density, tracer])
    near, far = edges(planes, sea_mask, mixed_level)
    near = lax.ppermute(near, "gx", [(i, i ^ 1) for i in range(ring)])
    far = lax.ppermute(far, "gx", [(i, (((i + 1) ^ 1) - 1) % ring) for i in range(ring)])
    packed = pack(planes, sea_mask, mixed_level, strips)
    packed = patch(near, far, packed, width)
    got = lax.all_to_all(packed, "gy", split_axis=0, concat_axis=0, tiled=True)
    done = sweeps(tile_blocks, block_owner, got.reshape(strips * blocks, VREGS, BR, LANES), width)
    back = lax.all_to_all(
        done.reshape(strips, -1, BR, LANES), "gy", split_axis=0, concat_axis=0, tiled=True
    )
    return unpack(back, rows, columns)


def solution(mesh):
    placed = (P(None, "gy", "gx"), P(None, "gy", "gx"), P("gy", "gx"), P("gy", "gx"), P(), P())
    return jax.shard_map(
        on_device, mesh=mesh, in_specs=placed, out_specs=P(None, "gy", "gx"), check_vma=False
    )
```

```python
import jax
import jax.numpy as jnp
from jax import lax
from jax.experimental import pallas as pl
from jax.experimental.pallas import tpu as pltpu
from jax.sharding import PartitionSpec as P

K = 8
BR = 8
ITERS = 4
HALO = ITERS + 1
LANES = 128
SLOTS = 3
VREGS = 6
UNPACK = 2
SMALL = 12 * 1024 * 1024
PLANES = 2 * K + 2
UNIT = 4
DEEPEST = 4
GATHER = 4
FACES = 44
SWEEP = 4
LAST = 4

TIME_STEP = 0.2
STRATIFICATION = 1.0
DENSITY_FLOOR = 0.25
SLOPE_LIMIT = 1.0
TAPER_WIDTH = 0.5
KERNEL_OFFSET = 0.05
BASE_DIFFUSIVITY = 0.2
VISBECK_ALPHA = 0.5


def rolled(x, shift):
    shift %= LANES
    return x if shift == 0 else pltpu.roll(x, shift, x.ndim - 1)


def lane_of(shape=(BR, LANES)):
    return lax.broadcasted_iota(jnp.int32, shape, len(shape) - 1)


def plane_at(register, piece):
    if piece == 2 and register == 2:
        return 2 * K
    if piece == 2 and register == 5:
        return 2 * K + 1
    return register % 3 + 3 * piece + (K if register >= 3 else 0)


def plane_of(planes, mask, mixed, p, rows, columns):
    if p < 2 * K:
        return planes[p, rows, columns]
    return (mask if p == 2 * K else mixed)[rows, columns].astype(jnp.float32)


def edges_kernel(planes, mask, mixed, near_ref, far_ref):
    shape = near_ref.shape
    lane = lane_of(shape)
    last = planes.shape[2] - LANES
    sides = []
    for start, edge in ((0, 0), (last, LANES - HALO)):
        out = jnp.zeros(shape, jnp.float32)
        for p in range(PLANES):
            at = HALO * p
            plane = plane_of(planes, mask, mixed, p, slice(None), slice(start, start + LANES))
            plane = rolled(plane, at - edge)
            out = jnp.where((lane >= at) & (lane < at + HALO), plane, out)
        sides.append(out)
    head, tail = sides
    even = lax.axis_index("gx") % 2 == 0
    near_ref[...] = jnp.where(even, tail, head)
    far_ref[...] = jnp.where(even, head, tail)


def edges(planes, mask, mixed):
    whole = pl.BlockSpec(memory_space=pltpu.VMEM)
    out = jax.ShapeDtypeStruct((planes.shape[1], LANES), jnp.float32)
    return pl.pallas_call(
        edges_kernel,
        out_shape=(out, out),
        in_specs=[whole, whole, whole],
        out_specs=(whole, whole),
        compiler_params=pltpu.CompilerParams(vmem_limit_bytes=SMALL),
        name="edges",
    )(planes, mask, mixed)


def pack_kernel(width, planes, mask, mixed, out_ref):
    piece = width + 2 * HALO
    per_tile = LANES // width
    tiles = planes.shape[2] // LANES
    lane = lane_of()

    def below(limit, start):
        return ((lane - start) & (LANES - 1)) < limit

    west_half = [below(LANES // 2, piece * m) for m in range(SLOTS)]
    one = [below(piece, width * q - HALO) for q in range(per_tile)]
    two = [below(2 * piece, width * q - HALO) for q in range(per_tile)]

    for b in range(planes.shape[1] // BR):
        for v in range(VREGS):
            whole, seam = [], []
            for m in range(SLOTS):
                own = [
                    rolled(
                        plane_of(
                            planes,
                            mask,
                            mixed,
                            plane_at(v, m),
                            slice(BR * b, BR * (b + 1)),
                            slice(LANES * t, LANES * (t + 1)),
                        ),
                        piece * m,
                    )
                    for t in range(tiles)
                ]
                whole.append(own)
                seam.append(
                    [own[0]]
                    + [jnp.where(west_half[m], own[t], own[t - 1]) for t in range(1, tiles)]
                    + [own[-1]]
                )
            for j in range(tiles * per_tile):
                t, q = divmod(j, per_tile)
                if q == 0:
                    parts = [seam[m][t] for m in range(SLOTS)]
                elif q == per_tile - 1:
                    parts = [seam[m][t + 1] for m in range(SLOTS)]
                else:
                    parts = [whole[m][t] for m in range(SLOTS)]
                out_ref[j, b * VREGS + v] = jnp.where(one[q], parts[0], jnp.where(two[q], parts[1], parts[2]))


def pack(planes, mask, mixed, strips):
    rows, columns = planes.shape[1:]
    whole = pl.BlockSpec(memory_space=pltpu.VMEM)
    width = columns // strips

    def kernel(*refs):
        pack_kernel(width, *refs)

    return pl.pallas_call(
        kernel,
        out_shape=jax.ShapeDtypeStruct((strips, rows // BR * VREGS, BR, LANES), jnp.float32),
        in_specs=[whole, whole, whole],
        out_specs=whole,
        compiler_params=pltpu.CompilerParams(vmem_limit_bytes=SMALL),
        cost_estimate=pl.CostEstimate(flops=20000000, bytes_accessed=6000000, transcendentals=0),
        name="pack",
    )(planes, mask, mixed)


def patch_kernel(width, near, far, packed, out_ref):
    piece = width + 2 * HALO
    even = lax.axis_index("gx") % 2 == 0
    lane = lane_of()
    strips = packed.shape[0]

    def fill(b, strip, evens, odds, start):
        here = slice(BR * b, BR * (b + 1))
        rim = jnp.where(even, evens[here, :], odds[here, :])
        for v in range(VREGS):
            value = packed[strip, b * VREGS + v]
            for m in range(SLOTS):
                at = (piece * m + start) % LANES
                here = (lane >= at) & (lane < at + HALO)
                value = jnp.where(here, rolled(rim, at - HALO * plane_at(v, m)), value)
            out_ref[strip, b * VREGS + v] = value

    for b in range(near.shape[0] // BR):
        fill(b, 0, far, near, LANES - HALO)
        fill(b, strips - 1, near, far, 0)


def patch(near, far, packed, width):
    whole = pl.BlockSpec(memory_space=pltpu.VMEM)

    def kernel(*refs):
        patch_kernel(width, *refs)

    return pl.pallas_call(
        kernel,
        out_shape=jax.ShapeDtypeStruct(packed.shape, jnp.float32),
        in_specs=[whole, whole, whole],
        out_specs=whole,
        input_output_aliases={2: 0},
        compiler_params=pltpu.CompilerParams(vmem_limit_bytes=SMALL),
        name="patch",
    )(near, far, packed)


def sweep_kernel(
    width, blocks, order, owner, got, out_ref, slot_of, rho, ta, tb, cp, cq, cr, sea, mix, kap, me, mw, mn, ms, ce, cw, cn, cs
):
    piece = width + 2 * HALO
    depth = (sea.shape[0] - 2 * BR) // BR
    strip = lax.axis_index("gy") % (LANES // width)

    def lane_from(start, shape=(BR, LANES)):
        return (lane_of(shape) - (width * strip + (start - HALO))) & (LANES - 1)

    lane = lane_from(0)
    first = lane < piece
    second = lane < 2 * piece

    def invert(s, carry):
        slot_of[order[s]] = s
        return carry

    lax.fori_loop(0, blocks, invert, 0, unroll=8)
    for b in range(blocks, SLOTS * depth):
        slot_of[b] = slot_of[0]

    def loop(body, count, chunk):
        def some(i, carry):
            body(i)
            return carry

        lax.fori_loop(0, count // chunk, some, 0)

    def rows(c, off=0, chunk=1):
        start = BR + BR * chunk * c
        if off == 0:
            return pl.ds(pl.multiple_of(start, BR), BR * chunk)
        return pl.ds(start + off, BR * chunk)

    def close(ref):
        top = jnp.where(first, 0.0, rolled(ref[pl.ds(BR * depth, BR), :], piece))
        bottom = jnp.where(second, rolled(ref[pl.ds(BR, BR), :], -piece), 0.0)
        ref[pl.ds(0, BR), :] = top
        ref[pl.ds(BR * (depth + 1), BR), :] = bottom

    def gather(c):
        for u in range(GATHER):
            i = c * GATHER + u
            slots = [slot_of[i + depth * m] for m in range(SLOTS)]
            owners = [owner[s] for s in slots]
            real = jnp.where(i + depth * (SLOTS - 1) < blocks, 1.0, 0.0)
            at = rows(i)
            for v in range(VREGS):
                where = slots if v < 3 else owners
                parts = [got[where[m], v] for m in range(SLOTS)]
                parts[2] = parts[2] * real
                for n in range(SLOTS):
                    moved = [rolled(parts[m], piece * (m - n)) for m in range(SLOTS)]
                    plane = jnp.where(first, moved[0], jnp.where(second, moved[1], moved[2]))
                    p = plane_at(v, n)
                    if p < K:
                        rho[p, at, :] = plane
                    elif p < 2 * K:
                        ta[p - K, at, :] = plane
                    elif p == 2 * K:
                        sea[at, :] = plane
            levels = [got[slots[m], 5] for m in range(SLOTS)]
            levels[2] = levels[2] * real
            levels = [rolled(levels[m], piece * (m - 2)) for m in range(SLOTS)]
            mix[at, :] = jnp.where(first, levels[0], jnp.where(second, levels[1], levels[2]))

    def physics(c):
        at, up, down = (rows(c, off, GATHER) for off in (0, 1, -1))
        mixed = mix[at, :]
        here = sea[at, :]
        east = rolled(here, -1) * here
        west = rolled(here, 1) * here
        north = sea[up, :] * here
        south = sea[down, :] * here
        me[at, :] = east
        mw[at, :] = west
        mn[at, :] = north
        ms[at, :] = south
        per_mixed = 1.0 / (mixed + 1.0)
        f = [rho[k, at, :] for k in range(K)]
        total = jnp.zeros_like(here)
        kept = []
        for k in range(K):
            sum_e = east * (rolled(f[k], -1) - f[k]) + west * (f[k] - rolled(f[k], 1))
            sum_n = north * (rho[k, up, :] - f[k]) + south * (f[k] - rho[k, down, :])
            above, under = max(k - 1, 0), min(k + 1, K - 1)
            rising = STRATIFICATION * (under - above)
            twice = jnp.maximum((f[under] - f[above]) + rising, 2.0 * DENSITY_FLOOR)
            scale = 1.0 / twice
            se = sum_e * scale
            sn = sum_n * scale
            squared = se * se + sn * sn
            taper = 1.0 + jnp.tanh(SLOPE_LIMIT / TAPER_WIDTH - squared * (1.0 / TAPER_WIDTH))
            if k < DEEPEST:
                taper = taper * jnp.minimum(1.0, (k + 1.0) * per_mixed)
            squared = squared * (taper * taper)
            under_root = twice * (squared + 4.0 * KERNEL_OFFSET)
            root = under_root * lax.rsqrt(under_root)
            total += jnp.where(mixed <= float(k), root, 0.0) if k < DEEPEST else root
            cp[k, at, :] = se * taper
            cq[k, at, :] = sn * taper
            kept.append(squared)
        share = (0.5 * VISBECK_ALPHA * 0.5**0.5) * total / (K - mixed)
        kappa = here * (BASE_DIFFUSIVITY + share)
        kap[at, :] = kappa
        weight = (0.25 * TIME_STEP) * kappa
        for k in range(K):
            cp[k, at, :] = -weight * cp[k, at, :]
            cq[k, at, :] = -weight * cq[k, at, :]
            cr[k, at, :] = (0.25 * weight) * kept[k]

    chunks = depth // GATHER

    def opening(i, carry):
        gather((i + chunks - 1) % chunks)
        return carry

    def both(c, carry):
        physics(c)
        gather(c + 2)
        return carry

    def closing(c, carry):
        physics(c)
        return carry

    lax.fori_loop(0, 3, opening, 0)
    for k in range(K):
        close(rho.at[k])
    close(sea)
    lax.fori_loop(0, chunks - 3, both, 0)
    lax.fori_loop(chunks - 3, chunks, closing, 0)
    for k in range(K):
        close(ta.at[k])
    close(kap)

    def faces(c):
        at, up, down = (rows(c, off, FACES) for off in (0, 1, -1))
        kappa = (0.5 * TIME_STEP) * kap[at, :]
        ce[at, :] = (kappa + rolled(kappa, -1)) * me[at, :]
        cw[at, :] = (kappa + rolled(kappa, 1)) * mw[at, :]
        cn[at, :] = (kappa + (0.5 * TIME_STEP) * kap[up, :]) * mn[at, :]
        cs[at, :] = (kappa + (0.5 * TIME_STEP) * kap[down, :]) * ms[at, :]

    loop(faces, depth, FACES)

    def advance(c, source, chunk):
        at, up, down = (rows(c, off, chunk) for off in (0, 1, -1))
        mask_e, mask_w, mask_n, mask_s = (ref[at, :] for ref in (me, mw, mn, ms))
        face_e, face_w, face_n, face_s = (ref[at, :] for ref in (ce, cw, cn, cs))
        f = [source[k, at, :] for k in range(K)]
        flux, result = [], []
        for k in range(K):
            step_e = rolled(f[k], -1) - f[k]
            step_w = f[k] - rolled(f[k], 1)
            step_n = source[k, up, :] - f[k]
            step_s = f[k] - source[k, down, :]
            sum_e = mask_e * step_e + mask_w * step_w
            sum_n = mask_n * step_n + mask_s * step_s
            lateral = (face_e * step_e - face_w * step_w) + (face_n * step_n - face_s * step_s)
            drop = f[min(k + 1, K - 1)] - f[max(k - 1, 0)]
            flux.append(cp[k, at, :] * sum_e + cq[k, at, :] * sum_n + cr[k, at, :] * drop)
            result.append(f[k] + lateral)
        for k in range(K):
            if k + 1 < K:
                result[k] += flux[k + 1]
            if k > 0:
                result[k] -= flux[k - 1]
        return result

    def sweep(source, target):
        def body(c):
            result = advance(c, source, SWEEP)
            for k in range(K):
                target[k, rows(c, 0, SWEEP), :] = result[k]

        loop(body, depth, SWEEP)
        for k in range(K):
            close(target.at[k])

    for n in range(ITERS - 1):
        sweep(*((ta, tb) if n % 2 == 0 else (tb, ta)))
    source = ta if (ITERS - 1) % 2 == 0 else tb
    per_out = LANES // width

    target = tb if source is ta else ta
    chunks = depth // LAST

    inner = [lane_from(piece * g + HALO, (BR * LAST, LANES)) for g in range(SLOTS)]

    def repack(c):
        for h in range(K // per_out):
            levels = [
                rolled(target[h * per_out + m, rows(c, 0, LAST), :], width * m) for m in range(per_out)
            ]
            for g in reversed(range(SLOTS)):
                value = levels[-1]
                for m in reversed(range(per_out - 1)):
                    value = jnp.where(inner[g] < width * (m + 1), levels[m], value)
                value = rolled(value, -piece * g)
                for u in range(LAST):
                    t = owner[slot_of[c * LAST + u + depth * g]]
                    out_ref[t, h] = value[BR * u : BR * (u + 1), :]

    def final(c):
        result = advance(c, source, LAST)
        for k in range(K):
            target[k, rows(c, 0, LAST), :] = result[k]

    def last(back, carry):
        repack(chunks - back)
        final(chunks - 1 - back)
        return carry

    final(chunks - 1)
    lax.fori_loop(1, chunks, last, 0)
    repack(0)


def sweeps(order, owner, got, width):
    blocks = got.shape[0]
    depth = -(-blocks // (SLOTS * UNIT)) * UNIT
    padded = BR * (depth + 2)
    cube = pltpu.VMEM((K, padded, LANES), jnp.float32)
    flat = pltpu.VMEM((padded, LANES), jnp.float32)
    outs = K * width // LANES

    def kernel(*refs):
        sweep_kernel(width, blocks, *refs)

    return pl.pallas_call(
        kernel,
        out_shape=jax.ShapeDtypeStruct((blocks, outs, BR, LANES), jnp.float32),
        in_specs=[
            pl.BlockSpec(memory_space=pltpu.SMEM),
            pl.BlockSpec(memory_space=pltpu.SMEM),
            pl.BlockSpec(memory_space=pltpu.VMEM),
        ],
        out_specs=pl.BlockSpec(memory_space=pltpu.VMEM),
        scratch_shapes=[pltpu.SMEM((SLOTS * depth,), jnp.int32)] + [cube] * 6 + [flat] * 11,
        compiler_params=pltpu.CompilerParams(vmem_limit_bytes=40 * 1024 * 1024),
        name="sweeps",
    )(order, owner, got)


def unpack_kernel(width, got, out_ref):
    per_tile = LANES // width
    tiles = out_ref.shape[2] // LANES
    count = out_ref.shape[1] // BR
    outs = K // per_tile
    place = lane_of() // width
    for u in range(count):
        block = pl.program_id(0) * count + u
        for h in range(outs):
            for t in range(tiles):
                strips = [got[t * per_tile + q, block * outs + h] for q in range(per_tile)]
                for m in range(per_tile):
                    value = strips[-1]
                    for q in range(per_tile - 1):
                        value = jnp.where(place == (m + q) % per_tile, strips[q], value)
                    out_ref[
                        h * per_tile + m, BR * u : BR * (u + 1), LANES * t : LANES * (t + 1)
                    ] = rolled(value, -width * m)


def unpack(got, rows, columns):
    strips = got.shape[0]
    blocks = rows // BR
    width = columns // strips

    def kernel(*refs):
        unpack_kernel(width, *refs)

    return pl.pallas_call(
        kernel,
        grid=(UNPACK,),
        out_shape=jax.ShapeDtypeStruct((K, rows, columns), jnp.float32),
        in_specs=[pl.BlockSpec(memory_space=pltpu.VMEM)],
        out_specs=pl.BlockSpec((K, rows // UNPACK, columns), lambda b: (0, b, 0)),
        compiler_params=pltpu.CompilerParams(vmem_limit_bytes=SMALL),
        name="unpack",
    )(got)


def on_device(density, tracer, sea_mask, mixed_level, tile_blocks, block_owner):
    rows, columns = sea_mask.shape
    strips = lax.axis_size("gy")
    ring = lax.axis_size("gx")
    width = columns // strips
    blocks = rows // BR
    planes = jnp.concatenate([density, tracer])
    near, far = edges(planes, sea_mask, mixed_level)
    near = lax.ppermute(near, "gx", [(i, i ^ 1) for i in range(ring)])
    far = lax.ppermute(far, "gx", [(i, (((i + 1) ^ 1) - 1) % ring) for i in range(ring)])
    packed = pack(planes, sea_mask, mixed_level, strips)
    packed = patch(near, far, packed, width)
    got = lax.all_to_all(packed, "gy", split_axis=0, concat_axis=0, tiled=True)
    done = sweeps(tile_blocks, block_owner, got.reshape(strips * blocks, VREGS, BR, LANES), width)
    back = lax.all_to_all(
        done.reshape(strips, -1, BR, LANES), "gy", split_axis=0, concat_axis=0, tiled=True
    )
    return unpack(back, rows, columns)


def solution(mesh):
    placed = (P(None, "gy", "gx"), P(None, "gy", "gx"), P("gy", "gx"), P("gy", "gx"), P(), P())
    return jax.shard_map(
        on_device, mesh=mesh, in_specs=placed, out_specs=P(None, "gy", "gx"), check_vma=False
    )
```

```python
import jax
import jax.numpy as jnp
from jax import lax
from jax.experimental import pallas as pl
from jax.experimental.pallas import tpu as pltpu
from jax.sharding import PartitionSpec as P

K = 8
BR = 8
ITERS = 4
HALO = ITERS + 1
LANES = 128
SLOTS = 3
VREGS = 6
UNPACK = 2
SMALL = 12 * 1024 * 1024
SPACING = 32 + 2 * HALO
UNIT = 4
DEEPEST = 4
GATHER = 4
FACES = 44
SWEEP = 4
LAST = 4

TIME_STEP = 0.2
STRATIFICATION = 1.0
DENSITY_FLOOR = 0.25
SLOPE_LIMIT = 1.0
TAPER_WIDTH = 0.5
KERNEL_OFFSET = 0.05
BASE_DIFFUSIVITY = 0.2
VISBECK_ALPHA = 0.5


def rolled(x, shift):
    shift %= LANES
    return x if shift == 0 else pltpu.roll(x, shift, x.ndim - 1)


def lane_of(shape=(BR, LANES)):
    return lax.broadcasted_iota(jnp.int32, shape, len(shape) - 1)


def plane_at(register, piece):
    if piece == 2 and register == 2:
        return 2 * K
    if piece == 2 and register == 5:
        return 2 * K + 1
    return register % 3 + 3 * piece + (K if register >= 3 else 0)


def plane_of(planes, mask, mixed, p, rows, columns):
    if p < 2 * K:
        return planes[p, rows, columns]
    return (mask if p == 2 * K else mixed)[rows, columns].astype(jnp.float32)


def edges_kernel(planes, mask, mixed, near_ref, far_ref):
    shape = near_ref.shape
    lane = lane_of(shape)
    last = planes.shape[2] - LANES
    sides = []
    for start, edge in ((0, 0), (last, LANES - HALO)):
        out = jnp.zeros(shape, jnp.float32)
        for v in range(VREGS):
            for m in range(SLOTS):
                at = SPACING * m + HALO * v
                plane = plane_of(planes, mask, mixed, plane_at(v, m), slice(None), slice(start, start + LANES))
                here = (lane >= at) & (lane < at + HALO)
                out = jnp.where(here, rolled(plane, at - edge), out)
        sides.append(out)
    head, tail = sides
    even = lax.axis_index("gx") % 2 == 0
    near_ref[...] = jnp.where(even, tail, head)
    far_ref[...] = jnp.where(even, head, tail)


def edges(planes, mask, mixed):
    whole = pl.BlockSpec(memory_space=pltpu.VMEM)
    out = jax.ShapeDtypeStruct((planes.shape[1], LANES), jnp.float32)
    return pl.pallas_call(
        edges_kernel,
        out_shape=(out, out),
        in_specs=[whole, whole, whole],
        out_specs=(whole, whole),
        compiler_params=pltpu.CompilerParams(vmem_limit_bytes=SMALL),
        name="edges",
    )(planes, mask, mixed)


def pack_kernel(width, planes, mask, mixed, out_ref):
    piece = width + 2 * HALO
    per_tile = LANES // width
    tiles = planes.shape[2] // LANES
    lane = lane_of()

    def below(limit, start):
        return ((lane - start) & (LANES - 1)) < limit

    west_half = [below(LANES // 2, piece * m) for m in range(SLOTS)]
    one = [below(piece, width * q - HALO) for q in range(per_tile)]
    two = [below(2 * piece, width * q - HALO) for q in range(per_tile)]

    for b in range(planes.shape[1] // BR):
        for v in range(VREGS):
            whole, seam = [], []
            for m in range(SLOTS):
                own = [
                    rolled(
                        plane_of(
                            planes,
                            mask,
                            mixed,
                            plane_at(v, m),
                            slice(BR * b, BR * (b + 1)),
                            slice(LANES * t, LANES * (t + 1)),
                        ),
                        piece * m,
                    )
                    for t in range(tiles)
                ]
                whole.append(own)
                seam.append(
                    [own[0]]
                    + [jnp.where(west_half[m], own[t], own[t - 1]) for t in range(1, tiles)]
                    + [own[-1]]
                )
            for j in range(tiles * per_tile):
                t, q = divmod(j, per_tile)
                if q == 0:
                    parts = [seam[m][t] for m in range(SLOTS)]
                elif q == per_tile - 1:
                    parts = [seam[m][t + 1] for m in range(SLOTS)]
                else:
                    parts = [whole[m][t] for m in range(SLOTS)]
                out_ref[j, b * VREGS + v] = jnp.where(one[q], parts[0], jnp.where(two[q], parts[1], parts[2]))


def pack(planes, mask, mixed, strips):
    rows, columns = planes.shape[1:]
    whole = pl.BlockSpec(memory_space=pltpu.VMEM)
    width = columns // strips

    def kernel(*refs):
        pack_kernel(width, *refs)

    return pl.pallas_call(
        kernel,
        out_shape=jax.ShapeDtypeStruct((strips, rows // BR * VREGS, BR, LANES), jnp.float32),
        in_specs=[whole, whole, whole],
        out_specs=whole,
        compiler_params=pltpu.CompilerParams(vmem_limit_bytes=SMALL),
        cost_estimate=pl.CostEstimate(flops=20000000, bytes_accessed=6000000, transcendentals=0),
        name="pack",
    )(planes, mask, mixed)


def patch_kernel(width, near, far, packed, out_ref):
    piece = width + 2 * HALO
    assert piece == SPACING
    even = lax.axis_index("gx") % 2 == 0
    lane = lane_of()
    strips = packed.shape[0]

    def fill(b, strip, evens, odds, start):
        here = slice(BR * b, BR * (b + 1))
        rim = jnp.where(even, evens[here, :], odds[here, :])
        hole = ((lane - start) & (LANES - 1)) < HALO
        for m in range(1, SLOTS):
            hole |= ((lane - (piece * m + start)) & (LANES - 1)) < HALO
        for v in range(VREGS):
            at = b * VREGS + v
            out_ref[strip, at] = jnp.where(hole, rolled(rim, start - HALO * v), packed[strip, at])

    for b in range(near.shape[0] // BR):
        fill(b, 0, far, near, LANES - HALO)
        fill(b, strips - 1, near, far, 0)


def patch(near, far, packed, width):
    whole = pl.BlockSpec(memory_space=pltpu.VMEM)

    def kernel(*refs):
        patch_kernel(width, *refs)

    return pl.pallas_call(
        kernel,
        out_shape=jax.ShapeDtypeStruct(packed.shape, jnp.float32),
        in_specs=[whole, whole, whole],
        out_specs=whole,
        input_output_aliases={2: 0},
        compiler_params=pltpu.CompilerParams(vmem_limit_bytes=SMALL),
        name="patch",
    )(near, far, packed)


def sweep_kernel(
    width, blocks, order, owner, got, out_ref, slot_of, rho, ta, tb, cp, cq, cr, sea, mix, kap, me, mw, mn, ms, ce, cw, cn, cs
):
    piece = width + 2 * HALO
    depth = (sea.shape[0] - 2 * BR) // BR
    strip = lax.axis_index("gy") % (LANES // width)

    def lane_from(start, shape=(BR, LANES)):
        return (lane_of(shape) - (width * strip + (start - HALO))) & (LANES - 1)

    lane = lane_from(0)
    first = lane < piece
    second = lane < 2 * piece

    def invert(s, carry):
        slot_of[order[s]] = s
        return carry

    lax.fori_loop(0, blocks, invert, 0, unroll=8)
    for b in range(blocks, SLOTS * depth):
        slot_of[b] = slot_of[0]

    def loop(body, count, chunk):
        def some(i, carry):
            body(i)
            return carry

        lax.fori_loop(0, count // chunk, some, 0)

    def rows(c, off=0, chunk=1):
        start = BR + BR * chunk * c
        if off == 0:
            return pl.ds(pl.multiple_of(start, BR), BR * chunk)
        return pl.ds(start + off, BR * chunk)

    def close(ref):
        top = jnp.where(first, 0.0, rolled(ref[pl.ds(BR * depth, BR), :], piece))
        bottom = jnp.where(second, rolled(ref[pl.ds(BR, BR), :], -piece), 0.0)
        ref[pl.ds(0, BR), :] = top
        ref[pl.ds(BR * (depth + 1), BR), :] = bottom

    def gather(c):
        for u in range(GATHER):
            i = c * GATHER + u
            slots = [slot_of[i + depth * m] for m in range(SLOTS)]
            owners = [owner[s] for s in slots]
            real = jnp.where(i + depth * (SLOTS - 1) < blocks, 1.0, 0.0)
            at = rows(i)
            for v in range(VREGS):
                where = slots if v < 3 else owners
                parts = [got[where[m], v] for m in range(SLOTS)]
                parts[2] = parts[2] * real
                for n in range(SLOTS):
                    moved = [rolled(parts[m], piece * (m - n)) for m in range(SLOTS)]
                    plane = jnp.where(first, moved[0], jnp.where(second, moved[1], moved[2]))
                    p = plane_at(v, n)
                    if p < K:
                        rho[p, at, :] = plane
                    elif p < 2 * K:
                        ta[p - K, at, :] = plane
                    elif p == 2 * K:
                        sea[at, :] = plane
            levels = [got[slots[m], 5] for m in range(SLOTS)]
            levels[2] = levels[2] * real
            levels = [rolled(levels[m], piece * (m - 2)) for m in range(SLOTS)]
            mix[at, :] = jnp.where(first, levels[0], jnp.where(second, levels[1], levels[2]))

    def physics(c):
        at, up, down = (rows(c, off, GATHER) for off in (0, 1, -1))
        mixed = mix[at, :]
        here = sea[at, :]
        east = rolled(here, -1) * here
        west = rolled(here, 1) * here
        north = sea[up, :] * here
        south = sea[down, :] * here
        me[at, :] = east
        mw[at, :] = west
        mn[at, :] = north
        ms[at, :] = south
        per_mixed = 1.0 / (mixed + 1.0)
        total = jnp.zeros_like(here)
        for k in range(K):
            f = rho[k, at, :]
            sum_e = east * (rolled(f, -1) - f) + west * (f - rolled(f, 1))
            sum_n = north * (rho[k, up, :] - f) + south * (f - rho[k, down, :])
            above, under = max(k - 1, 0), min(k + 1, K - 1)
            rising = STRATIFICATION * (under - above)
            twice = jnp.maximum((rho[under, at, :] - rho[above, at, :]) + rising, 2.0 * DENSITY_FLOOR)
            scale = 1.0 / twice
            se = sum_e * scale
            sn = sum_n * scale
            squared = se * se + sn * sn
            taper = 1.0 + jnp.tanh(SLOPE_LIMIT / TAPER_WIDTH - squared * (1.0 / TAPER_WIDTH))
            if k < DEEPEST:
                taper = taper * jnp.minimum(1.0, (k + 1.0) * per_mixed)
            squared = squared * (taper * taper)
            under_root = twice * (squared + 4.0 * KERNEL_OFFSET)
            root = under_root * lax.rsqrt(under_root)
            total += jnp.where(mixed <= float(k), root, 0.0) if k < DEEPEST else root
            cp[k, at, :] = se * taper
            cq[k, at, :] = sn * taper
            cr[k, at, :] = squared
        share = (0.5 * VISBECK_ALPHA * 0.5**0.5) * total / (K - mixed)
        kappa = here * (BASE_DIFFUSIVITY + share)
        kap[at, :] = kappa
        weight = (0.25 * TIME_STEP) * kappa
        for k in range(K):
            cp[k, at, :] = -weight * cp[k, at, :]
            cq[k, at, :] = -weight * cq[k, at, :]
            cr[k, at, :] = (0.25 * weight) * cr[k, at, :]

    chunks = depth // GATHER

    def opening(i, carry):
        gather((i + chunks - 1) % chunks)
        return carry

    def both(c, carry):
        physics(c)
        gather(c + 2)
        return carry

    def closing(c, carry):
        physics(c)
        return carry

    lax.fori_loop(0, 3, opening, 0)
    for k in range(K):
        close(rho.at[k])
    close(sea)
    lax.fori_loop(0, chunks - 3, both, 0)
    lax.fori_loop(chunks - 3, chunks, closing, 0)
    for k in range(K):
        close(ta.at[k])
    close(kap)

    def faces(c):
        at, up, down = (rows(c, off, FACES) for off in (0, 1, -1))
        kappa = (0.5 * TIME_STEP) * kap[at, :]
        ce[at, :] = (kappa + rolled(kappa, -1)) * me[at, :]
        cw[at, :] = (kappa + rolled(kappa, 1)) * mw[at, :]
        cn[at, :] = (kappa + (0.5 * TIME_STEP) * kap[up, :]) * mn[at, :]
        cs[at, :] = (kappa + (0.5 * TIME_STEP) * kap[down, :]) * ms[at, :]

    loop(faces, depth, FACES)

    def advance(c, source, chunk):
        at, up, down = (rows(c, off, chunk) for off in (0, 1, -1))
        mask_e, mask_w, mask_n, mask_s = (ref[at, :] for ref in (me, mw, mn, ms))
        face_e, face_w, face_n, face_s = (ref[at, :] for ref in (ce, cw, cn, cs))
        f = [source[k, at, :] for k in range(K)]
        flux, result = [], []
        for k in range(K):
            step_e = rolled(f[k], -1) - f[k]
            step_w = f[k] - rolled(f[k], 1)
            step_n = source[k, up, :] - f[k]
            step_s = f[k] - source[k, down, :]
            sum_e = mask_e * step_e + mask_w * step_w
            sum_n = mask_n * step_n + mask_s * step_s
            lateral = (face_e * step_e - face_w * step_w) + (face_n * step_n - face_s * step_s)
            drop = f[min(k + 1, K - 1)] - f[max(k - 1, 0)]
            flux.append(cp[k, at, :] * sum_e + cq[k, at, :] * sum_n + cr[k, at, :] * drop)
            result.append(f[k] + lateral)
        for k in range(K):
            if k + 1 < K:
                result[k] += flux[k + 1]
            if k > 0:
                result[k] -= flux[k - 1]
        return result

    def sweep(source, target):
        def body(c):
            result = advance(c, source, SWEEP)
            for k in range(K):
                target[k, rows(c, 0, SWEEP), :] = result[k]

        loop(body, depth, SWEEP)
        for k in range(K):
            close(target.at[k])

    for n in range(ITERS - 1):
        sweep(*((ta, tb) if n % 2 == 0 else (tb, ta)))
    source = ta if (ITERS - 1) % 2 == 0 else tb
    per_out = LANES // width

    target = tb if source is ta else ta
    chunks = depth // LAST

    inner = [lane_from(piece * g + HALO, (BR * LAST, LANES)) for g in range(SLOTS)]

    def repack(c):
        for h in range(K // per_out):
            levels = [
                rolled(target[h * per_out + m, rows(c, 0, LAST), :], width * m) for m in range(per_out)
            ]
            for g in reversed(range(SLOTS)):
                value = levels[-1]
                for m in reversed(range(per_out - 1)):
                    value = jnp.where(inner[g] < width * (m + 1), levels[m], value)
                value = rolled(value, -piece * g)
                for u in range(LAST):
                    t = owner[slot_of[c * LAST + u + depth * g]]
                    out_ref[t, h] = value[BR * u : BR * (u + 1), :]

    def final(c):
        result = advance(c, source, LAST)
        for k in range(K):
            target[k, rows(c, 0, LAST), :] = result[k]

    def last(back, carry):
        repack(chunks - back)
        final(chunks - 1 - back)
        return carry

    final(chunks - 1)
    lax.fori_loop(1, chunks, last, 0)
    repack(0)


def sweeps(order, owner, got, width):
    blocks = got.shape[0]
    depth = -(-blocks // (SLOTS * UNIT)) * UNIT
    padded = BR * (depth + 2)
    cube = pltpu.VMEM((K, padded, LANES), jnp.float32)
    flat = pltpu.VMEM((padded, LANES), jnp.float32)
    outs = K * width // LANES

    def kernel(*refs):
        sweep_kernel(width, blocks, *refs)

    return pl.pallas_call(
        kernel,
        out_shape=jax.ShapeDtypeStruct((blocks, outs, BR, LANES), jnp.float32),
        in_specs=[
            pl.BlockSpec(memory_space=pltpu.SMEM),
            pl.BlockSpec(memory_space=pltpu.SMEM),
            pl.BlockSpec(memory_space=pltpu.VMEM),
        ],
        out_specs=pl.BlockSpec(memory_space=pltpu.VMEM),
        scratch_shapes=[pltpu.SMEM((SLOTS * depth,), jnp.int32)] + [cube] * 6 + [flat] * 11,
        compiler_params=pltpu.CompilerParams(vmem_limit_bytes=40 * 1024 * 1024),
        name="sweeps",
    )(order, owner, got)


def unpack_kernel(width, got, out_ref):
    per_tile = LANES // width
    tiles = out_ref.shape[2] // LANES
    count = out_ref.shape[1] // BR
    outs = K // per_tile
    place = lane_of() // width
    for u in range(count):
        block = pl.program_id(0) * count + u
        for h in range(outs):
            for t in range(tiles):
                strips = [got[t * per_tile + q, block * outs + h] for q in range(per_tile)]
                for m in range(per_tile):
                    value = strips[-1]
                    for q in range(per_tile - 1):
                        value = jnp.where(place == (m + q) % per_tile, strips[q], value)
                    out_ref[
                        h * per_tile + m, BR * u : BR * (u + 1), LANES * t : LANES * (t + 1)
                    ] = rolled(value, -width * m)


def unpack(got, rows, columns):
    strips = got.shape[0]
    blocks = rows // BR
    width = columns // strips

    def kernel(*refs):
        unpack_kernel(width, *refs)

    return pl.pallas_call(
        kernel,
        grid=(UNPACK,),
        out_shape=jax.ShapeDtypeStruct((K, rows, columns), jnp.float32),
        in_specs=[pl.BlockSpec(memory_space=pltpu.VMEM)],
        out_specs=pl.BlockSpec((K, rows // UNPACK, columns), lambda b: (0, b, 0)),
        compiler_params=pltpu.CompilerParams(vmem_limit_bytes=SMALL),
        name="unpack",
    )(got)


def on_device(density, tracer, sea_mask, mixed_level, tile_blocks, block_owner):
    rows, columns = sea_mask.shape
    strips = lax.axis_size("gy")
    ring = lax.axis_size("gx")
    width = columns // strips
    blocks = rows // BR
    planes = jnp.concatenate([density, tracer])
    near, far = edges(planes, sea_mask, mixed_level)
    near = lax.ppermute(near, "gx", [(i, i ^ 1) for i in range(ring)])
    far = lax.ppermute(far, "gx", [(i, (((i + 1) ^ 1) - 1) % ring) for i in range(ring)])
    packed = pack(planes, sea_mask, mixed_level, strips)
    packed = patch(near, far, packed, width)
    got = lax.all_to_all(packed, "gy", split_axis=0, concat_axis=0, tiled=True)
    done = sweeps(tile_blocks, block_owner, got.reshape(strips * blocks, VREGS, BR, LANES), width)
    back = lax.all_to_all(
        done.reshape(strips, -1, BR, LANES), "gy", split_axis=0, concat_axis=0, tiled=True
    )
    return unpack(back, rows, columns)


def solution(mesh):
    placed = (P(None, "gy", "gx"), P(None, "gy", "gx"), P("gy", "gx"), P("gy", "gx"), P(), P())
    return jax.shard_map(
        on_device, mesh=mesh, in_specs=placed, out_specs=P(None, "gy", "gx"), check_vma=False
    )
```
